128 devices in a mesh: dp: 4 (over x), seq: 32 (over z, y, core).
Axes of the slice: x: 4, y: 4, z: 4, core: 2. Of those that a mesh axis runs over, the one named last changes fastest.
Arguments:
- tokens: bfloat16 [4, 8192, 2560], P('dp', 'seq'), may hold values from -6 to 6
- values: bfloat16 [4, 8192, 5120], P('dp', 'seq'), may hold values from -6 to 6
- out_grad: bfloat16 [4, 8192, 5120], P('dp', 'seq'), may hold values from -0.0007324219 to 0.0007324219
- w_bc: bfloat16 [2560, 256], replicated, may hold values from -0.009765625 to 0.009765625
- w_dt: bfloat16 [2560, 80], replicated, may hold values from -0.125 to 0.125
- a_log: float32 [80], replicated, may hold values from -13 to -2
- dt_bias: float32 [80], replicated, may hold values from -1 to 1
- fire_flags: int32 [4], P('dp'), may hold values from 0 to 1, as said below
- last_bc: float32 [4, 2560, 256], P('dp', 'seq'), may hold values from -27 to 27
- last_heads: float32 [4, 2, 80], P('dp'), may hold values from -6 to 6
- total_bc: float32 [2560, 256], P('seq'), may hold values from -6 to 6
- total_heads: float32 [2, 80], replicated, may hold values from -6 to 6
Outputs:
- new_total_bc: float32 [2560, 256], P('seq')
- new_total_heads: float32 [2, 80], replicated
- new_last_bc: float32 [4, 2560, 256], P('dp', 'seq')
- new_last_heads: float32 [4, 2, 80], P('dp')
- trigger: float32 [4], P('dp')
The draws below stay inside these ranges and needn't reach their ends.
Inputs may be any that keep to these rules, and one draw needn't show every extreme that they name: `fire_flags`: between 2 and 3 entries are 1; which ones varies.
All inputs are finite; a program needn't handle non-finite values.
Results may differ from the reference program's by a relative error of at most 0.0029.
Values sent between devices are 32-bit elements; how exact they have to be, the bound alone decides.
No kernel may reach another device: no remote copies, remote signals or barrier semaphores. Data moves between devices by JAX's collectives and lax.ppermute only.
A program may use at most 320 MiB of HBM per device.

```python
import jax
import jax.numpy as jnp
from jax import lax

D = 2560
N = 128
H = 80
P_SIZE = 64
GROUP = 128
REPLICAS = 4
LENGTH = 8192


def draw_a_log(key, part):
    base_key = jax.random.fold_in(key, 101)
    pick_key, slow_key, fast_key = jax.random.split(base_key, 3)
    quick_heads = jax.random.permutation(pick_key, H) < H // 2
    slow_rate = jnp.exp(jax.random.uniform(slow_key, (H,), jnp.float32, jnp.log(0.3), jnp.log(2.0))) / LENGTH
    fast_rate = jnp.exp(jax.random.uniform(fast_key, (H,), jnp.float32, jnp.log(0.02), jnp.log(0.1)))
    return jnp.log(jnp.where(quick_heads, fast_rate, slow_rate)).astype(jnp.float32)


def draw_fire_flags(key, part):
    base_key = jax.random.fold_in(key, 202)
    count_key, order_key = jax.random.split(base_key, 2)
    fire_count = jax.random.randint(count_key, (), 2, REPLICAS)
    ranking = jax.random.permutation(order_key, REPLICAS)
    return (ranking < fire_count).astype(jnp.int32)


def draw_last_bc(key, part):
    base_key = jax.random.fold_in(key, 303)
    noise = jax.random.truncated_normal(base_key, -6.0, 6.0, (REPLICAS, D, 2 * N), jnp.float32)
    position = jnp.arange(D, dtype=jnp.float32) / (D - 1)
    row_scale = 0.5 * (1.0 + 2.0 * position)
    return (noise * row_scale[None, :, None]).astype(jnp.float32)


def strengthened(values, rng, source, target, parts, factor):
    owner, partner = [(jnp.arange(values.shape[dim]) // (values.shape[dim] // parts)).reshape([-1 if axis == dim else 1 for axis in range(values.ndim)]) for dim in (source, target)]
    chosen = jax.random.permutation(rng, parts)[partner]
    strong = (owner == chosen) | (owner == (partner + parts // 2) % parts)
    return jnp.where(strong, factor * values, values)


def level_of(stream_key, extent, shards, least, largest):
    def one(axis_at, blocks):
        steps = jax.random.uniform(jax.random.fold_in(jax.random.fold_in(stream_key, 6), axis_at), (blocks,), jnp.float32, least / len(shards), largest / len(shards))
        return jnp.repeat(jnp.exp(steps), extent[axis_at] // blocks).reshape((-1,) + (1,) * (len(extent) - axis_at - 1))

    loudness = one(*shards[0])
    for cut in shards[1:]:
        loudness = loudness * one(*cut)
    return loudness


def scatter_about(own_key, shape, width, reach, cuts=(), kind=jnp.bfloat16):
    factor_of = level_of(own_key, shape, cuts, -0.22, 0.18) if cuts else 1.0
    values = jax.random.normal(own_key, shape, jnp.float32) * width * factor_of
    return jnp.minimum(jnp.maximum(values, -reach), reach).astype(kind)


def noise_with(stream_key, extent, deviation, limit, shards, heavy, kind=jnp.bfloat16):
    drawn = deviation * jax.random.normal(stream_key, extent, jnp.float32)
    if shards:
        drawn = drawn * level_of(stream_key, extent, shards, -0.22, 0.18)
    return jnp.clip(strengthened(drawn, jax.random.fold_in(stream_key, 3), *heavy), -limit, limit).astype(kind)


def setup_inputs(seed: int = 0) -> dict:
    key_of = jax.random.split(jax.random.key(seed), 13)
    tokens = noise_with(key_of[0], (REPLICAS, LENGTH, D), 1.0, 6.0, ((0, 4), (1, 32)), (1, 2, 32, 2.75))
    values = scatter_about(key_of[1], (REPLICAS, LENGTH, H * P_SIZE), 1.0, 6.0, ((0, 4), (1, 32)))
    out_grad = scatter_about(key_of[2], (REPLICAS, LENGTH, H * P_SIZE), (1.0 / LENGTH), 0.0007324219, ((0, 4), (1, 32)))
    w_bc = scatter_about(key_of[3], (D, 2 * N), (D * N) ** -0.5, 0.009765625)
    w_dt = scatter_about(key_of[4], (D, H), D ** -0.5, 0.125)
    a_log = draw_a_log(jax.random.fold_in(key_of[12], 71), 0)
    dt_bias = jnp.clip(jax.random.uniform(key_of[6], (H,), jnp.float32, -1.0, 1.0), -1.0, 1.0)
    fire_flags = draw_fire_flags(jax.random.fold_in(key_of[12], 71), 0)
    last_bc = draw_last_bc(jax.random.fold_in(key_of[12], 71), 0)
    last_heads = scatter_about(key_of[9], (REPLICAS, 2, H), 1.0, 6.0, ((0, 4),), jnp.float32)
    total_bc = scatter_about(key_of[10], (D, 2 * N), 1.0, 6.0, ((0, 32),), jnp.float32)
    total_heads = scatter_about(key_of[11], (2, H), 1.0, 6.0, (), jnp.float32)
    return dict(tokens=tokens, values=values, out_grad=out_grad, w_bc=w_bc, w_dt=w_dt, a_log=a_log, dt_bias=dt_bias, fire_flags=fire_flags, last_bc=last_bc, last_heads=last_heads, total_bc=total_bc, total_heads=total_heads)


HIGHEST = lax.Precision.HIGHEST

def project_heads(projected, raw_dt, a_log, dt_bias):
    half_width = projected.shape[1] // 2
    step_rates = jax.nn.softplus(raw_dt + dt_bias)
    log_decay = -step_rates * jnp.exp(a_log)
    return (projected[:, :half_width], projected[:, half_width:], step_rates, log_decay)

def group_terms(carried, pieces):
    state_now, loss_sum = carried
    value_rows, b_rows, c_rows, step_rates, log_decay, grad_rows = pieces
    block_len, head_count = step_rates.shape
    values_full = value_rows.astype(jnp.float32).reshape(block_len, head_count, -1)
    grads_full = grad_rows.astype(jnp.float32).reshape(block_len, head_count, -1)
    cumulated = jnp.cumsum(log_decay, axis=0)
    decay_gap = cumulated.T[:, :, None] - cumulated.T[:, None, :]
    causal = lax.broadcasted_iota(jnp.int32, (block_len, block_len), 0) >= lax.broadcasted_iota(jnp.int32, (block_len, block_len), 1)
    decay_mat = jnp.exp(jnp.where(causal[None], decay_gap, -1e+30))
    scores = jnp.dot(c_rows, b_rows.T, precision=HIGHEST)
    mix_weights = decay_mat * scores[None] * step_rates.T[:, None, :]
    inside = jnp.einsum('hts,shp->thp', mix_weights, values_full, precision=HIGHEST)
    outside = jnp.einsum('tn,hnp->thp', c_rows, state_now, precision=HIGHEST) * jnp.exp(cumulated)[:, :, None]
    loss_sum = loss_sum + jnp.sum((inside + outside) * grads_full)
    tail_weight = jnp.exp(cumulated[-1] - cumulated) * step_rates
    fresh = jnp.einsum('sn,shp->hnp', b_rows, tail_weight[:, :, None] * values_full, precision=HIGHEST)
    state_now = jnp.exp(cumulated[-1])[:, None, None] * state_now + fresh
    return ((state_now, loss_sum), None)

def in_blocks(array):
    blocks = array.shape[0] // GROUP
    return array.reshape((blocks, GROUP) + array.shape[1:])

def sequence_loss(state_start, value_rows, b_rows, c_rows, step_rates, log_decay, grad_rows):
    pieces = (in_blocks(value_rows), in_blocks(b_rows), in_blocks(c_rows), in_blocks(step_rates), in_blocks(log_decay), in_blocks(grad_rows))
    carried, unused = lax.scan(jax.checkpoint(group_terms), (state_start, jnp.zeros((), jnp.float32)), pieces)
    return carried[1]

def replica_grads(tok_rows, value_rows, grad_rows, w_bc, w_dt, a_log, dt_bias):
    projected = jnp.dot(tok_rows, w_bc, preferred_element_type=jnp.float32)
    raw_dt = jnp.dot(tok_rows, w_dt, preferred_element_type=jnp.float32)

    def loss_of(projected, a_log, dt_bias):
        b_rows, c_rows, step_rates, log_decay = project_heads(projected, raw_dt, a_log, dt_bias)
        state_start = jnp.zeros((H, N, P_SIZE), jnp.float32)
        return sequence_loss(state_start, value_rows, b_rows, c_rows, step_rates, log_decay, grad_rows)
    loss_proj, loss_alog, loss_bias = jax.grad(loss_of, argnums=(0, 1, 2))(projected, a_log, dt_bias)
    grad_bc = jnp.einsum('td,tk->dk', tok_rows, loss_proj.astype(jnp.bfloat16), preferred_element_type=jnp.float32)
    return (grad_bc, jnp.stack([loss_alog, loss_bias]))

def reference(tokens, values, out_grad, w_bc, w_dt, a_log, dt_bias, fire_flags, last_bc, last_heads, total_bc, total_heads):
    fired_bc = jnp.zeros_like(total_bc)
    fired_heads = jnp.zeros_like(total_heads)
    kept_bc = []
    kept_heads = []
    norms = []
    for replica in range(REPLICAS):
        grad_bc, grad_heads = replica_grads(tokens[replica], values[replica], out_grad[replica], w_bc, w_dt, a_log, dt_bias)
        diff_bc = grad_bc - last_bc[replica]
        diff_heads = grad_heads - last_heads[replica]
        norms.append(jnp.sqrt(jnp.sum(diff_bc * diff_bc) + jnp.sum(diff_heads * diff_heads) + 1e-06))
        weight = fire_flags[replica].astype(jnp.float32)
        fired_bc = fired_bc + weight * diff_bc
        fired_heads = fired_heads + weight * diff_heads
        kept_bc.append(jnp.where(fire_flags[replica] > 0, grad_bc, last_bc[replica]))
        kept_heads.append(jnp.where(fire_flags[replica] > 0, grad_heads, last_heads[replica]))
    return (total_bc + fired_bc, total_heads + fired_heads, jnp.stack(kept_bc), jnp.stack(kept_heads), jnp.stack(norms))
```

```python
import jax
import jax.numpy as jnp
from jax import lax
from jax.experimental import pallas as pl
from jax.experimental.pallas import tpu as pltpu
from jax.sharding import Mesh
from jax.sharding import PartitionSpec as P

F32 = jnp.float32
BF16 = jnp.bfloat16
T = 256
D = 2560
N = 128
HEADS = 80
W = 5120
HALF = 64
CHIPS = 16
SEQ = ("z", "y", "c")
RING = ("z", "y")
CORE_SWAP = [(0, 1), (1, 0)]


def iota(shape, dim):
    return lax.broadcasted_iota(jnp.int32, shape, dim)


def halves(x):
    high = x.astype(BF16)
    return high, (x - high.astype(F32)).astype(BF16)


def thirds(x):
    high = x.astype(BF16)
    rest = x - high.astype(F32)
    mid = rest.astype(BF16)
    return high, mid, (rest - mid.astype(F32)).astype(BF16)


def mm(a, b):
    return jnp.dot(a, b, preferred_element_type=F32)


def mm_nt(a, b):
    return lax.dot_general(a, b, (((1,), (1,)), ((), ())), preferred_element_type=F32)


def mm_tn(a, b):
    return lax.dot_general(a, b, (((0,), (0,)), ((), ())), preferred_element_type=F32)


def spread_matrix(first_head, lanes):
    head = iota((256, lanes), 0) % 128
    return (head == first_head + iota((256, lanes), 1) // 64).astype(BF16)


def gather_matrix(first_head, lanes):
    return (first_head + iota((lanes, 128), 0) // 64 == iota((lanes, 128), 1)).astype(BF16)


def paired(x):
    return jnp.concatenate(halves(x), axis=1)


def whole(shape):
    return pl.BlockSpec(shape, lambda *_: (0,) * len(shape))


SCALARS = pl.BlockSpec(memory_space=pltpu.SMEM)


def params(*semantics):
    return pltpu.CompilerParams(dimension_semantics=semantics, vmem_limit_bytes=48 << 20)


def project_kernel(
    core, tok, w_bc, w_dt, a_log, dt_bias,
    b_out, c_out, bt_out, ct_out, tail_out, grow_out, cum3_out, cum_t_out, rate_t_out, heads_out, end_out,
    acc_bc, acc_dt, row,
):
    step = pl.program_id(0)

    @pl.when(step == 0)
    def _():
        acc_bc[...] = jnp.zeros_like(acc_bc)
        acc_dt[...] = jnp.zeros_like(acc_dt)
        row[...] = jnp.zeros_like(row)
        row[0:1, 0:HEADS] = a_log[...]
        row[8:9, 0:HEADS] = dt_bias[...]

    u = tok[...]
    acc_bc[...] += mm(u, w_bc[...])
    acc_dt[:, 0:HEADS] += mm(u, w_dt[...])

    @pl.when(step == pl.num_programs(0) - 1)
    def _():
        second = core[0] == 1
        b = acc_bc[:, 0:N]
        c = acc_bc[:, N : 2 * N]
        b = jnp.where(second, pltpu.roll(b, HALF, 1), b)
        c = jnp.where(second, pltpu.roll(c, HALF, 1), c)
        b_out[...] = b
        c_out[...] = c
        bt_hi, bt_lo = halves(b.T)
        ct_hi, ct_lo = halves(c.T)
        bt_out[0:N, :] = bt_hi
        bt_out[N : 2 * N, :] = bt_lo
        ct_out[0:N, :] = ct_hi
        ct_out[N : 2 * N, :] = ct_lo
        x = acc_dt[...] + row[8:9, :]
        small = jnp.exp(-jnp.abs(x))
        rate = jnp.maximum(x, 0.0) + jnp.log1p(small)
        slope = jnp.where(x >= 0.0, 1.0, small) / (1.0 + small)
        pace = jnp.exp(row[0:1, :])
        decay = -rate * pace
        upto = (iota((T, T), 0) >= iota((T, T), 1)).astype(BF16)
        d0, d1, d2 = thirds(decay)
        cum = mm(upto, d2) + mm(upto, d1) + mm(upto, d0)
        end = cum[T - 1 : T, :]
        tail_out[...] = paired(jnp.exp(end - cum) * rate)
        grow_out[...] = paired(jnp.exp(cum))
        c0, c1, c2 = thirds(cum)
        cum3_out[:, 0:128] = c0
        cum3_out[:, 128:256] = c1
        cum3_out[:, 256:384] = c2
        cum_t_out[...] = cum.T
        rate_t_out[...] = rate.T
        heads_out[0] = decay
        heads_out[1] = -pace * slope
        heads_out[2] = jnp.where(rate > 0.0, slope / rate, 0.0)
        end_out[...] = jnp.broadcast_to(end, (8, 128))


def project(core, tok, w_bc, w_dt, a_log, dt_bias):
    steps = 5
    k = D // steps
    shape = jax.ShapeDtypeStruct
    outs = (
        shape((T, N), F32), shape((T, N), F32), shape((2 * N, T), BF16), shape((2 * N, T), BF16),
        shape((T, 256), BF16), shape((T, 256), BF16), shape((T, 384), BF16),
        shape((128, T), F32), shape((128, T), F32), shape((3, T, 128), F32), shape((8, 128), F32),
    )
    return pl.pallas_call(
        project_kernel,
        grid=(steps,),
        in_specs=[
            SCALARS,
            pl.BlockSpec((T, k), lambda i: (0, i)),
            pl.BlockSpec((k, 2 * N), lambda i: (i, 0)),
            pl.BlockSpec((k, HEADS), lambda i: (i, 0)),
            whole((1, HEADS)),
            whole((1, HEADS)),
        ],
        out_specs=[whole(o.shape) for o in outs],
        out_shape=outs,
        scratch_shapes=[pltpu.VMEM((T, 2 * N), F32), pltpu.VMEM((T, 128), F32), pltpu.VMEM((16, 128), F32)],
        compiler_params=params("arbitrary"),
        name="project",
    )(core, tok, w_bc, w_dt, a_log, dt_bias)


LANES = 256
STEPS = W // LANES


def scaled(pair, spread, rows):
    return mm(pair, spread) * rows.astype(F32)


def three(left, right):
    hi, lo = halves(right)
    return mm(left[0:N], hi) + (mm(left[0:N], lo) + mm(left[N : 2 * N], hi))


def summary_kernel(v, g, tail, grow, bt, ct, own, other):
    spread = spread_matrix(pl.program_id(0) * (LANES // 64), LANES)
    fresh = three(bt, scaled(tail[...], spread, v[...]))
    own[0:HALF, :] = fresh[0:HALF]
    other[0:HALF, :] = fresh[HALF:N]
    entry = three(ct, scaled(grow[...], spread, g[...]))
    own[HALF:N, :] = entry[0:HALF]
    other[HALF:N, :] = entry[HALF:N]


def summary(v, g, tail, grow, bt, ct):
    lanes = pl.BlockSpec((T, LANES), lambda i: (0, i))
    out = pl.BlockSpec((N, LANES), lambda i: (0, i))
    return pl.pallas_call(
        summary_kernel,
        grid=(STEPS,),
        in_specs=[lanes, lanes, whole((T, 256)), whole((T, 256)), whole((2 * N, T)), whole((2 * N, T))],
        out_specs=[out, out],
        out_shape=[jax.ShapeDtypeStruct((N, W), F32)] * 2,
        compiler_params=params("arbitrary"),
        name="summary",
    )(v, g, tail, grow, bt, ct)


def chip_kernel(core, own, arrived, end, end_other, out):
    second = core[0] == 1
    mine = jnp.exp(end[...])
    theirs = jnp.exp(end_other[...])
    one = jnp.ones_like(mine)
    weights = jnp.concatenate(
        [
            jnp.where(second, one, theirs),
            jnp.where(second, mine, one),
            jnp.where(second, theirs, one),
            jnp.where(second, one, mine),
        ],
        axis=0,
    )
    weights = paired(weights)
    upper = iota((8, 512), 0) < 4
    for lane in range(0, W, 512):
        s = slice(lane, lane + 512)
        scale = mm(weights, spread_matrix(lane // 64, 512))
        for k in range(8):
            r = slice(8 * k, 8 * k + 8)
            q = slice(HALF + 8 * k, HALF + 8 * k + 8)
            fwd = scale[0:8] * own[r, s] + scale[8:16] * arrived[r, s]
            bwd = scale[16:24] * own[q, s] + scale[24:32] * arrived[q, s]
            out[2 * k, :, s] = jnp.where(upper, fwd, pltpu.roll(bwd, 4, 0))
            out[2 * k + 1, :, s] = jnp.where(upper, pltpu.roll(fwd, 4, 0), bwd)
    total = end[...] + end_other[...]
    for k in range(CHIPS):
        out[k, :, W : W + 128] = total


def chip_terms(core, own, arrived, end, end_other):
    return pl.pallas_call(
        chip_kernel,
        in_specs=[SCALARS] + [pl.BlockSpec(memory_space=pltpu.VMEM)] * 4,
        out_specs=pl.BlockSpec(memory_space=pltpu.VMEM),
        out_shape=jax.ShapeDtypeStruct((CHIPS, 8, W + 128), F32),
        compiler_params=pltpu.CompilerParams(vmem_limit_bytes=48 << 20),
        name="chip_terms",
    )(core, own, arrived, end, end_other)


SCAN_LANES = 1024


def scan_kernel(terms, ends, out):
    width = SCAN_LANES
    decays = paired(jnp.exp(ends[...].reshape(CHIPS * 8, 128)))
    first = pl.program_id(0) * (width // 64)
    upper = iota((8, 512), 0) < 4
    for lane in range(0, width, 512):
        s = slice(lane, lane + 512)
        decay = mm(decays, spread_matrix(first + lane // 64, 512))
        state = jnp.zeros((8, 512), F32)
        for k in range(CHIPS):
            m = CHIPS - 1 - k
            out[k, 0:4, s] = state[0:4]
            out[m, 4:8, s] = state[4:8]
            here = jnp.where(upper, terms[k, :, s], terms[m, :, s])
            rate = jnp.where(upper, decay[8 * k : 8 * k + 8], decay[8 * m : 8 * m + 8])
            state = rate * state + here


def scan_chips(terms):
    return pl.pallas_call(
        scan_kernel,
        grid=(W // SCAN_LANES,),
        in_specs=[
            pl.BlockSpec((CHIPS, 8, SCAN_LANES), lambda i: (0, 0, i)),
            pl.BlockSpec((CHIPS, 8, 128), lambda i: (0, 0, W // 128)),
        ],
        out_specs=pl.BlockSpec((CHIPS, 8, SCAN_LANES), lambda i: (0, 0, i)),
        out_shape=jax.ShapeDtypeStruct((CHIPS, 8, W), F32),
        compiler_params=params("arbitrary"),
        name="scan_chips",
    )(terms, terms)


def cores_kernel(core, states, own, arrived, end, end_other, mine_out, send_out):
    width = SCAN_LANES
    second = core[0] == 1
    mine = jnp.exp(end[...])
    theirs = jnp.exp(end_other[...])
    one = jnp.ones_like(mine)
    zero = jnp.zeros_like(mine)
    pick0 = jnp.where(second, zero, one)
    pick1 = jnp.where(second, one, zero)
    weights = paired(
        jnp.concatenate(
            [
                jnp.where(second, theirs, one),
                jnp.where(second, one, mine),
                jnp.where(second, one, theirs),
                jnp.where(second, mine, one),
                pick0,
                pick1,
            ],
            axis=0,
        )
    )
    first = pl.program_id(0) * (width // 64)
    upper = iota((8, 512), 0) < 4
    for lane in range(0, width, 512):
        s = slice(lane, lane + 512)
        w = mm(weights, spread_matrix(first + lane // 64, 512))
        for k in range(8):
            r = slice(8 * k, 8 * k + 8)
            q = slice(HALF + 8 * k, HALF + 8 * k + 8)
            even = states[2 * k, :, s]
            odd = states[2 * k + 1, :, s]
            fwd = jnp.where(upper, even, pltpu.roll(odd, 4, 0))
            bwd = jnp.where(upper, pltpu.roll(even, 4, 0), odd)
            mine_out[r, s] = w[0:8] * fwd + w[40:48] * arrived[r, s]
            send_out[r, s] = w[8:16] * fwd + w[32:40] * own[r, s]
            mine_out[q, s] = w[16:24] * bwd + w[32:40] * arrived[q, s]
            send_out[q, s] = w[24:32] * bwd + w[40:48] * own[q, s]


def core_states(core, states, own, arrived, end, end_other):
    rows = pl.BlockSpec((N, SCAN_LANES), lambda i: (0, i))
    return pl.pallas_call(
        cores_kernel,
        grid=(W // SCAN_LANES,),
        in_specs=[
            SCALARS,
            pl.BlockSpec((CHIPS, 8, SCAN_LANES), lambda i: (0, 0, i)),
            rows,
            rows,
            whole((8, 128)),
            whole((8, 128)),
        ],
        out_specs=[rows, rows],
        out_shape=[jax.ShapeDtypeStruct((N, W), F32)] * 2,
        compiler_params=params("arbitrary"),
        name="core_states",
    )(core, states, own, arrived, end, end_other)


INSIDE_LANES = 512


def inside_kernel(v, g, b, c, cum3, cum_t, rate_t, db_out, dc_out, row_out, col_out, mix, scores):
    step = pl.program_id(0)

    @pl.when(step == 0)
    def _():
        c_hi, c_lo = halves(c[...])
        b_hi, b_lo = halves(b[...])
        scores[...] = mm_nt(c_hi, b_hi) + (mm_nt(c_hi, b_lo) + mm_nt(c_lo, b_hi))
        mix[...] = jnp.zeros_like(mix)
        row_out[...] = jnp.zeros_like(row_out)

    causal = iota((128, 128), 0) >= iota((128, 128), 1)
    left = iota((T, 128), 1) < 64
    per_step = INSIDE_LANES // 64
    pick = iota((384, 128), 0) % 128 == step * per_step + iota((384, 128), 1)
    cols = mm(cum3[...], pick.astype(BF16))
    lane = iota((128, 128), 1)
    sums0 = row_out[0:128, :]
    sums1 = row_out[128:256, :]
    zero = jnp.zeros((), BF16)
    for j in range(per_step):
        head = step * per_step + j
        pair = slice(128 * (j // 2), 128 * (j // 2) + 128)
        v_pair = v[:, pair]
        g_pair = g[:, pair]
        g_head = jnp.where(left if j % 2 == 0 else ~left, g_pair, zero)
        cum_row = cum_t[j : j + 1, :]
        rate_row = rate_t[j : j + 1, :]

        def block(t0, s0):
            t = slice(t0, t0 + 128)
            s = slice(s0, s0 + 128)
            gap = cols[t, j : j + 1] - cum_row[:, s]
            if t0 == s0:
                gap = jnp.where(causal, gap, -1e30)
            part = jnp.exp(gap) * rate_row[:, s] * mm_nt(g_head[t], v_pair[s])
            mix[t, s] += part
            return part * scores[t, s]

        m00 = block(0, 0)
        m10 = block(128, 0)
        m11 = block(128, 128)
        sums0 = jnp.where(lane == head, jnp.sum(m00, axis=1, keepdims=True), sums0)
        sums1 = jnp.where(lane == head, jnp.sum(m10 + m11, axis=1, keepdims=True), sums1)
        col_out[j : j + 1, 0:128] = jnp.sum(m00 + m10, axis=0, keepdims=True)
        col_out[j : j + 1, 128:256] = jnp.sum(m11, axis=0, keepdims=True)
    row_out[0:128, :] = sums0
    row_out[128:256, :] = sums1

    @pl.when(step == pl.num_programs(0) - 1)
    def _():
        m_hi, m_lo = halves(mix[...])
        b_hi, b_lo = halves(b[...])
        c_hi, c_lo = halves(c[...])
        dc_out[...] = mm(m_hi, b_hi) + (mm(m_hi, b_lo) + mm(m_lo, b_hi))
        db_out[...] = mm_tn(m_hi, c_hi) + (mm_tn(m_hi, c_lo) + mm_tn(m_lo, c_hi))


def inside(v, g, b, c, cum3, cum_t, rate_t):
    lanes = pl.BlockSpec((T, INSIDE_LANES), lambda i: (0, i))
    some = pl.BlockSpec((INSIDE_LANES // 64, T), lambda i: (i, 0))
    shape = jax.ShapeDtypeStruct
    outs = (shape((T, N), F32), shape((T, N), F32), shape((T, 128), F32), shape((128, T), F32))
    return pl.pallas_call(
        inside_kernel,
        grid=(W // INSIDE_LANES,),
        in_specs=[lanes, lanes, whole((T, N)), whole((T, N)), whole((T, 384)), some, some],
        out_specs=[whole((T, N)), whole((T, N)), whole((T, 128)), some],
        out_shape=outs,
        scratch_shapes=[pltpu.VMEM((T, T), F32), pltpu.VMEM((T, T), F32)],
        compiler_params=params("arbitrary"),
        cost_estimate=pl.CostEstimate(flops=20_000_000_000, transcendentals=4_000_000, bytes_accessed=6_000_000),
        name="inside",
    )(v, g, b, c, cum3, cum_t, rate_t)


def outside_kernel(v, g, mine, got, tail, grow, b, c, db_out, dc_out, x_out, z_out, link_out):
    step = pl.program_id(0)
    first = step * (LANES // 64)

    @pl.when(step == 0)
    def _():
        for ref in (db_out, dc_out, x_out, z_out, link_out):
            ref[...] = jnp.zeros_like(ref)

    spread = spread_matrix(first, LANES)
    gather = gather_matrix(first, LANES)
    state_in = jnp.concatenate([mine[0:HALF, :], got[0:HALF, :]], axis=0)
    state_back = jnp.concatenate([mine[HALF:N, :], got[HALF:N, :]], axis=0)

    def side(pair, rows, state, other, d_out, sum_out):
        weighted = scaled(pair[...], spread, rows[...])
        s_hi, s_lo = halves(state)
        w_hi, w_lo = halves(weighted)
        o_hi, o_lo = halves(other[...])
        d_out[...] += mm_nt(w_hi, s_hi) + (mm_nt(w_hi, s_lo) + mm_nt(w_lo, s_hi))
        reached = mm(o_hi, s_hi) + (mm(o_hi, s_lo) + mm(o_lo, s_hi))
        p_hi, p_lo = halves(weighted * reached)
        sum_out[...] += mm(p_hi, gather) + mm(p_lo, gather)

    side(grow, g, state_in, c, dc_out, x_out)
    side(tail, v, state_back, b, db_out, z_out)
    joint = jnp.broadcast_to(jnp.sum(state_in * state_back, axis=0, keepdims=True), (8, LANES))
    j0, j1, j2 = thirds(joint)
    link_out[...] += mm(j0, gather) + (mm(j1, gather) + mm(j2, gather))


def outside(v, g, mine, got, tail, grow, b, c):
    lanes = pl.BlockSpec((T, LANES), lambda i: (0, i))
    rows = pl.BlockSpec((N, LANES), lambda i: (0, i))
    shape = jax.ShapeDtypeStruct
    outs = (
        shape((T, N), F32), shape((T, N), F32), shape((T, 128), F32), shape((T, 128), F32), shape((8, 128), F32),
    )
    return pl.pallas_call(
        outside_kernel,
        grid=(STEPS,),
        in_specs=[lanes, lanes, rows, rows, whole((T, 256)), whole((T, 256)), whole((T, N)), whole((T, N))],
        out_specs=[whole(o.shape) for o in outs],
        out_shape=outs,
        compiler_params=params("arbitrary"),
        name="outside",
    )(v, g, mine, got, tail, grow, b, c)


GRAD_STEPS = 4
GRAD_ROWS = D // GRAD_STEPS
ROWS = D // 32


def grads_kernel(
    core, tok, db_in, dc_in, db_far, dc_far, rows_in, cols_in, x_far, z_far, link, end, heads,
    own, other, heads_out,
    d_proj, res,
):
    step = pl.program_id(0)
    which = core[0]

    @pl.when(step == 0)
    def _():
        second = which == 1
        db = db_in[...] + db_far[...]
        dc = dc_in[...] + dc_far[...]
        d_proj[:, 0:N] = jnp.where(second, pltpu.roll(db, HALF, 1), db).astype(BF16)
        d_proj[:, N : 2 * N] = jnp.where(second, pltpu.roll(dc, HALF, 1), dc).astype(BF16)
        z = z_far[...]
        ahead = rows_in[...] + x_far[...]
        behind = jnp.where(iota((T, 128), 1) < HEADS, cols_in[...].T, 0.0) + z
        d0, d1, d2 = thirds(ahead - behind)
        onward = (iota((T, T), 0) <= iota((T, T), 1)).astype(BF16)
        carry = jnp.exp(end[0:1, :]) * link[0:1, :] + jnp.sum(z, axis=0, keepdims=True)
        flux = mm(onward, d0) + (mm(onward, d1) + mm(onward, d2)) + carry
        d_log = jnp.sum(flux * heads[0], axis=0, keepdims=True)
        d_bias = jnp.sum(behind * heads[2] + flux * heads[1], axis=0, keepdims=True)
        heads_out[0:1, :] = d_log
        heads_out[1:2, :] = d_bias
        heads_out[2:8, :] = jnp.zeros((6, 128), F32)

    res[...] = mm_tn(tok[...], d_proj[...])
    for k in range(GRAD_ROWS // (2 * ROWS)):
        own[k] = res[pl.ds(2 * ROWS * k + ROWS * which, ROWS), :]
        other[k] = res[pl.ds(2 * ROWS * k + ROWS * (1 - which), ROWS), :]


def grads(core, tok, *parts):
    shape = jax.ShapeDtypeStruct
    pieces = GRAD_ROWS // (2 * ROWS)
    out = pl.BlockSpec((pieces, ROWS, 2 * N), lambda i: (i, 0, 0))
    return pl.pallas_call(
        grads_kernel,
        grid=(GRAD_STEPS,),
        in_specs=[SCALARS, pl.BlockSpec((T, GRAD_ROWS), lambda i: (0, i))] + [whole(p.shape) for p in parts],
        out_specs=[out, out, whole((8, 128))],
        out_shape=[shape((CHIPS, ROWS, 2 * N), F32)] * 2 + [shape((8, 128), F32)],
        scratch_shapes=[pltpu.VMEM((T, 2 * N), BF16), pltpu.VMEM((GRAD_ROWS, 2 * N), F32)],
        compiler_params=params("arbitrary"),
        name="grads",
    )(core, tok, *parts)


def all_to_all(x, axis):
    return lax.all_to_all(x, axis, 0, 0, tiled=True)


def from_everyone(x, axis, count):
    return all_to_all(jnp.broadcast_to(x[None], (count, *x.shape)), axis)


def local(
    tokens, values, out_grad, w_bc, w_dt, a_log, dt_bias, fire_flags, last_bc, last_heads, total_bc, total_heads
):
    tok, v, g = tokens[0], values[0], out_grad[0]
    core = lax.axis_index("c").astype(jnp.int32).reshape(1)
    b, c, bt, ct, tail, grow, cum3, cum_t, rate_t, heads, end = project(
        core, tok, w_bc, w_dt, a_log.reshape(1, HEADS), dt_bias.reshape(1, HEADS)
    )
    end_other = lax.ppermute(end, "c", CORE_SWAP)
    own, other = summary(v, g, tail, grow, bt, ct)
    arrived = lax.ppermute(other, "c", CORE_SWAP)
    terms = chip_terms(core, own, arrived, end, end_other)
    gathered = all_to_all(terms, RING)
    db_in, dc_in, rows_in, cols_in = inside(v, g, b, c, cum3, cum_t, rate_t)
    states = all_to_all(scan_chips(gathered), RING)
    mine, send = core_states(core, states, own, arrived, end, end_other)
    got = lax.ppermute(send, "c", CORE_SWAP)
    db_far, dc_far, x_far, z_far, link = outside(v, g, mine, got, tail, grow, b, c)
    rows_own, rows_other, grad_heads = grads(
        core, tok, db_in, dc_in, db_far, dc_far, rows_in, cols_in, x_far, z_far, link, end, heads
    )
    all_heads = from_everyone(grad_heads[0:2, 0:HEADS], SEQ, 32)
    rows = rows_own + lax.ppermute(rows_other, "c", CORE_SWAP)
    own_rows = jnp.sum(all_to_all(rows, RING), axis=0)
    summed_heads = jnp.sum(all_heads, axis=0)
    fired = fire_flags[0] > 0
    weight = fire_flags[0].astype(F32)
    diff_bc = own_rows - last_bc[0]
    diff_heads = summed_heads - last_heads[0]
    square = jnp.sum(from_everyone(jnp.sum(diff_bc * diff_bc).reshape(1), SEQ, 32))
    trigger = jnp.sqrt(square + jnp.sum(diff_heads * diff_heads) + 1e-06)
    packed = jnp.concatenate([(weight * diff_bc).reshape(-1), (weight * diff_heads).reshape(-1)])
    fired_sum = jnp.sum(from_everyone(packed, "dp", 4), axis=0)
    cut = ROWS * 2 * N
    return (
        total_bc + fired_sum[:cut].reshape(ROWS, 2 * N),
        total_heads + fired_sum[cut:].reshape(2, HEADS),
        jnp.where(fired, own_rows, last_bc[0])[None],
        jnp.where(fired, summed_heads, last_heads[0])[None],
        trigger.reshape(1),
    )


def solution(mesh):
    split = Mesh(mesh.devices.reshape(mesh.shape["dp"], 4, 4, 2), ("dp",) + SEQ)
    rows = P("dp", SEQ, None)
    in_specs = (
        rows, rows, rows, P(), P(), P(), P(), P("dp"), rows, P("dp", None, None), P(SEQ, None), P(),
    )
    out_specs = (P(SEQ, None), P(), rows, P("dp", None, None), P("dp"))
    return jax.shard_map(local, mesh=split, in_specs=in_specs, out_specs=out_specs, check_vma=False)
```

```python
import functools

import jax
import jax.numpy as jnp
from jax import lax
from jax.experimental import pallas as pl
from jax.experimental.pallas import tpu as pltpu
from jax.sharding import Mesh
from jax.sharding import PartitionSpec as P

F32 = jnp.float32
BF16 = jnp.bfloat16
T = 256
D = 2560
N = 128
HEADS = 80
W = 5120
HALF = 64
CHIPS = 16
SEQ = ("z", "y", "c")
RING = ("z", "y")
CORE_SWAP = [(0, 1), (1, 0)]


def iota(shape, dim):
    return lax.broadcasted_iota(jnp.int32, shape, dim)


def halves(x):
    high = x.astype(BF16)
    return high, (x - high.astype(F32)).astype(BF16)


def thirds(x):
    high = x.astype(BF16)
    rest = x - high.astype(F32)
    mid = rest.astype(BF16)
    return high, mid, (rest - mid.astype(F32)).astype(BF16)


def mm(a, b):
    return jnp.dot(a, b, preferred_element_type=F32)


def mm_nt(a, b):
    return lax.dot_general(a, b, (((1,), (1,)), ((), ())), preferred_element_type=F32)


def mm_tn(a, b):
    return lax.dot_general(a, b, (((0,), (0,)), ((), ())), preferred_element_type=F32)


def spread_matrix(first_head, lanes):
    head = iota((256, lanes), 0) % 128
    return (head == first_head + iota((256, lanes), 1) // 64).astype(BF16)


def gather_matrix(first_head, lanes):
    return (first_head + iota((lanes, 128), 0) // 64 == iota((lanes, 128), 1)).astype(BF16)


def paired(x):
    return jnp.concatenate(halves(x), axis=1)


def whole(shape):
    return pl.BlockSpec(shape, lambda *_: (0,) * len(shape))


SCALARS = pl.BlockSpec(memory_space=pltpu.SMEM)


def params(*semantics):
    return pltpu.CompilerParams(dimension_semantics=semantics, vmem_limit_bytes=20 << 20)


LANES = 256
STEPS = W // LANES


def scaled(pair, spread, rows):
    return mm(pair, spread) * rows.astype(F32)


def three(left, right):
    hi, lo = halves(right)
    return mm(left[0:N], hi) + (mm(left[0:N], lo) + mm(left[N : 2 * N], hi))


PARTS = 5
PART_D = D // PARTS
PART_W = W // PARTS
IN_HBM = pl.BlockSpec(memory_space=pltpu.HBM)
IN_VMEM = pl.BlockSpec(memory_space=pltpu.VMEM)


def cut(i, width):
    return slice(i * width, (i + 1) * width)


def front_kernel(
    core, tok, w_bc, w_dt, a_log, dt_bias, v, g,
    own, other, b_out, c_out, tail_out, grow_out, cum3_out, cum_t_out, rate_t_out, heads_out, end_out,
    tok_buf, bc_buf, dt_buf, log_buf, bias_buf, v_buf, g_buf, own_buf, other_buf, row, wide, bt, ct,
    tok_sem, bc_sem, dt_sem, row_sem, v_sem, g_sem, out_sem,
):
    copies = []
    for i in range(PARTS):
        k = cut(i, PART_D)
        copies.append((
            pltpu.make_async_copy(tok.at[:, k], tok_buf.at[i], tok_sem.at[i]),
            pltpu.make_async_copy(w_bc.at[k, :], bc_buf.at[i], bc_sem.at[i]),
            pltpu.make_async_copy(w_dt.at[:, k], dt_buf.at[i], dt_sem.at[i]),
        ))
    small = (
        pltpu.make_async_copy(a_log, log_buf, row_sem.at[0]),
        pltpu.make_async_copy(dt_bias, bias_buf, row_sem.at[1]),
    )
    rows_in = [
        (
            pltpu.make_async_copy(v.at[:, cut(i, PART_W)], v_buf.at[i], v_sem.at[i]),
            pltpu.make_async_copy(g.at[:, cut(i, PART_W)], g_buf.at[i], g_sem.at[i]),
        )
        for i in range(PARTS)
    ]
    for group in copies:
        for copy in group:
            copy.start()
    for copy in small:
        copy.start()
    for group in rows_in:
        for copy in group:
            copy.start()
    row[...] = jnp.zeros_like(row)
    wide[...] = jnp.zeros_like(wide)
    projected = None
    raw_dt = None
    for i in range(PARTS):
        for copy in copies[i]:
            copy.wait()
        u = tok_buf[i]
        part = mm(u, bc_buf[i])
        part_dt = mm_nt(u, dt_buf[i])
        projected = part if i == 0 else projected + part
        raw_dt = part_dt if i == 0 else raw_dt + part_dt
    for copy in small:
        copy.wait()
    row[0:1, 0:HEADS] = log_buf[...]
    row[8:9, 0:HEADS] = bias_buf[...]
    wide[:, 0:HEADS] = raw_dt
    second = core[0] == 1
    b = projected[:, 0:N]
    c = projected[:, N : 2 * N]
    b = jnp.where(second, pltpu.roll(b, HALF, 1), b)
    c = jnp.where(second, pltpu.roll(c, HALF, 1), c)
    b_out[...] = b
    c_out[...] = c
    bt_hi, bt_lo = halves(b.T)
    ct_hi, ct_lo = halves(c.T)
    bt[0:N, :] = bt_hi
    bt[N : 2 * N, :] = bt_lo
    ct[0:N, :] = ct_hi
    ct[N : 2 * N, :] = ct_lo
    x = wide[...] + row[8:9, :]
    small_exp = jnp.exp(-jnp.abs(x))
    rate = jnp.maximum(x, 0.0) + jnp.log1p(small_exp)
    slope = jnp.where(x >= 0.0, 1.0, small_exp) / (1.0 + small_exp)
    pace = jnp.exp(row[0:1, :])
    decay = -rate * pace
    upto = (iota((T, T), 0) >= iota((T, T), 1)).astype(BF16)
    d0, d1, d2 = thirds(decay)
    cum = mm(upto, d2) + mm(upto, d1) + mm(upto, d0)
    end = cum[T - 1 : T, :]
    tail_out[...] = paired(jnp.exp(end - cum) * rate)
    grow_out[...] = paired(jnp.exp(cum))
    c0, c1, c2 = thirds(cum)
    cum3_out[:, 0:128] = c0
    cum3_out[:, 128:256] = c1
    cum3_out[:, 256:384] = c2
    cum_t_out[...] = cum.T
    rate_t_out[...] = rate.T
    heads_out[0] = decay
    heads_out[1] = -pace * slope
    heads_out[2] = jnp.where(rate > 0.0, slope / rate, 0.0)
    end_out[...] = jnp.broadcast_to(end, (8, 128))
    outs = []
    for i in range(PARTS):
        for copy in rows_in[i]:
            copy.wait()
        for lane in range(0, PART_W, LANES):
            s = slice(lane, lane + LANES)
            spread = spread_matrix((i * PART_W + lane) // 64, LANES)
            fresh = three(bt, scaled(tail_out[...], spread, v_buf[i, :, s]))
            entry = three(ct, scaled(grow_out[...], spread, g_buf[i, :, s]))
            own_buf[i, 0:HALF, s] = fresh[0:HALF]
            own_buf[i, HALF:N, s] = entry[0:HALF]
            other_buf[i, 0:HALF, s] = fresh[HALF:N]
            other_buf[i, HALF:N, s] = entry[HALF:N]
        for n, (src, dst) in enumerate(((other_buf, other), (own_buf, own))):
            copy = pltpu.make_async_copy(src.at[i], dst.at[:, cut(i, PART_W)], out_sem.at[n, i])
            copy.start()
            outs.append(copy)
    for copy in outs:
        copy.wait()


def front(core, tok, w_bc, w_dt, a_log, dt_bias, v, g):
    shape = jax.ShapeDtypeStruct
    vmem = pltpu.VMEM
    dma = pltpu.SemaphoreType.DMA
    small_outs = (
        shape((T, N), F32), shape((T, N), F32), shape((T, 256), BF16), shape((T, 256), BF16), shape((T, 384), BF16),
        shape((128, T), F32), shape((128, T), F32), shape((3, T, 128), F32), shape((8, 128), F32),
    )
    tok, w_bc, w_dt, a_log, dt_bias, v, g = (
        pltpu.with_memory_space_constraint(x, pltpu.HBM) for x in (tok, w_bc, w_dt, a_log, dt_bias, v, g)
    )
    return pl.pallas_call(
        front_kernel,
        in_specs=[SCALARS] + [IN_HBM] * 7,
        out_specs=[IN_HBM] * 2 + [whole(o.shape) for o in small_outs],
        out_shape=(pltpu.HBM((N, W), F32),) * 2 + tuple(pltpu.HBM(o.shape, o.dtype) for o in small_outs),
        scratch_shapes=[
            vmem((PARTS, T, PART_D), BF16), vmem((PARTS, PART_D, 2 * N), BF16), vmem((PARTS, HEADS, PART_D), BF16),
            vmem((1, HEADS), F32), vmem((1, HEADS), F32),
            vmem((PARTS, T, PART_W), BF16), vmem((PARTS, T, PART_W), BF16),
            vmem((PARTS, N, PART_W), F32), vmem((PARTS, N, PART_W), F32),
            vmem((16, 128), F32), vmem((T, 128), F32), vmem((2 * N, T), BF16), vmem((2 * N, T), BF16),
            dma((PARTS,)), dma((PARTS,)), dma((PARTS,)), dma((2,)), dma((PARTS,)), dma((PARTS,)), dma((2, PARTS)),
        ],
        compiler_params=pltpu.CompilerParams(vmem_limit_bytes=28 << 20),
        name="front",
    )(core, tok, w_bc, w_dt, a_log, dt_bias, v, g)


def chip_kernel(core, own, arrived, end, end_other, out, kept, own_buf, out_buf, own_sem, keep_sem, out_sem):
    ins = [pltpu.make_async_copy(own.at[:, cut(i, PART_W)], own_buf.at[i], own_sem.at[i]) for i in range(PARTS)]
    for copy in ins:
        copy.start()
    keep = pltpu.make_async_copy(arrived, kept, keep_sem)
    keep.start()
    second = core[0] == 1
    mine = jnp.exp(end[...])
    theirs = jnp.exp(end_other[...])
    one = jnp.ones_like(mine)
    weights = jnp.concatenate(
        [
            jnp.where(second, one, theirs),
            jnp.where(second, mine, one),
            jnp.where(second, theirs, one),
            jnp.where(second, one, mine),
        ],
        axis=0,
    )
    weights = paired(weights)
    upper = iota((8, 512), 0) < 4
    total = end[...] + end_other[...]
    for k in range(CHIPS):
        out_buf[k, :, W : W + 128] = total
    outs = []
    for i in range(PARTS):
        ins[i].wait()
        for lane in range(0, PART_W, 512):
            s = slice(lane, lane + 512)
            to = slice(i * PART_W + lane, i * PART_W + lane + 512)
            scale = mm(weights, spread_matrix((i * PART_W + lane) // 64, 512))
            for k in range(8):
                r = slice(8 * k, 8 * k + 8)
                q = slice(HALF + 8 * k, HALF + 8 * k + 8)
                fwd = scale[0:8] * own_buf[i, r, s] + scale[8:16] * arrived[r, to]
                bwd = scale[16:24] * own_buf[i, q, s] + scale[24:32] * arrived[q, to]
                out_buf[2 * k, :, to] = jnp.where(upper, fwd, pltpu.roll(bwd, 4, 0))
                out_buf[2 * k + 1, :, to] = jnp.where(upper, pltpu.roll(fwd, 4, 0), bwd)
        lanes = slice(i * PART_W, (i + 1) * PART_W + (128 if i == PARTS - 1 else 0))
        copy = pltpu.make_async_copy(out_buf.at[:, :, lanes], out.at[:, :, lanes], out_sem.at[i])
        copy.start()
        outs.append(copy)
    for copy in outs:
        copy.wait()
    keep.wait()


def chip_terms(core, own, arrived, end, end_other):
    dma = pltpu.SemaphoreType.DMA
    return pl.pallas_call(
        chip_kernel,
        in_specs=[SCALARS, IN_HBM] + [IN_VMEM] * 3,
        out_specs=[IN_HBM] * 2,
        out_shape=[pltpu.HBM((CHIPS, 8, W + 128), F32), pltpu.HBM((N, W), F32)],
        scratch_shapes=[
            pltpu.VMEM((PARTS, N, PART_W), F32), pltpu.VMEM((CHIPS, 8, W + 128), F32),
            dma((PARTS,)), dma(()), dma((PARTS,)),
        ],
        compiler_params=params(),
        name="chip_terms",
    )(core, pltpu.with_memory_space_constraint(own, pltpu.HBM), arrived, end, end_other)


SCAN_LANES = 1024


def scan_kernel(terms, ends, after, out):
    width = SCAN_LANES
    decays = paired(jnp.exp(ends[...].reshape(CHIPS * 8, 128)))
    first = pl.program_id(0) * (width // 64)
    upper = iota((8, 512), 0) < 4
    for lane in range(0, width, 512):
        s = slice(lane, lane + 512)
        decay = mm(decays, spread_matrix(first + lane // 64, 512))
        state = jnp.zeros((8, 512), F32)
        for k in range(CHIPS):
            m = CHIPS - 1 - k
            out[k, 0:4, s] = state[0:4]
            out[m, 4:8, s] = state[4:8]
            here = jnp.where(upper, terms[k, :, s], terms[m, :, s])
            rate = jnp.where(upper, decay[8 * k : 8 * k + 8], decay[8 * m : 8 * m + 8])
            state = rate * state + here


def scan_chips(terms, after):
    return pl.pallas_call(
        scan_kernel,
        grid=(W // SCAN_LANES,),
        in_specs=[
            pl.BlockSpec((CHIPS, 8, SCAN_LANES), lambda i: (0, 0, i)),
            pl.BlockSpec((CHIPS, 8, 128), lambda i: (0, 0, W // 128)),
            pl.BlockSpec(memory_space=pl.ANY),
        ],
        out_specs=pl.BlockSpec((CHIPS, 8, SCAN_LANES), lambda i: (0, 0, i)),
        out_shape=jax.ShapeDtypeStruct((CHIPS, 8, W), F32),
        compiler_params=params("arbitrary"),
        name="scan_chips",
    )(terms, terms, after)


def core_kernel(sending, core, states, part, end, end_other, out):
    width = SCAN_LANES
    first_core = (core[0] == 0) == sending
    decay = jnp.exp(jnp.where(sending, end[...], end_other[...]))
    one = jnp.ones_like(decay)
    zero = jnp.zeros_like(decay)
    weights = paired(
        jnp.concatenate(
            [
                jnp.where(first_core, decay, one) if sending else jnp.where(first_core, decay, one),
                jnp.where(first_core, one, zero),
                jnp.where(first_core, one, decay),
                jnp.where(first_core, zero, one),
            ],
            axis=0,
        )
    )
    first = pl.program_id(0) * (width // 64)
    upper = iota((8, 512), 0) < 4
    for lane in range(0, width, 512):
        s = slice(lane, lane + 512)
        w = mm(weights, spread_matrix(first + lane // 64, 512))
        for k in range(8):
            r = slice(8 * k, 8 * k + 8)
            q = slice(HALF + 8 * k, HALF + 8 * k + 8)
            even = states[2 * k, :, s]
            odd = states[2 * k + 1, :, s]
            fwd = jnp.where(upper, even, pltpu.roll(odd, 4, 0))
            bwd = jnp.where(upper, pltpu.roll(even, 4, 0), odd)
            out[r, s] = w[0:8] * fwd + w[8:16] * part[r, s]
            out[q, s] = w[16:24] * bwd + w[24:32] * part[q, s]


def core_states(sending, core, states, part, end, end_other):
    rows = pl.BlockSpec((N, SCAN_LANES), lambda i: (0, i))
    return pl.pallas_call(
        functools.partial(core_kernel, sending),
        grid=(W // SCAN_LANES,),
        in_specs=[
            SCALARS,
            pl.BlockSpec((CHIPS, 8, SCAN_LANES), lambda i: (0, 0, i)),
            rows,
            whole((8, 128)),
            whole((8, 128)),
        ],
        out_specs=rows,
        out_shape=jax.ShapeDtypeStruct((N, W), F32),
        compiler_params=params("arbitrary"),
        cost_estimate=pl.CostEstimate(flops=2_000_000_000, transcendentals=0, bytes_accessed=8_000_000),
        name="sent_states" if sending else "own_states",
    )(core, states, part, end, end_other)


INSIDE_LANES = 512


def inside_kernel(v, g, b, c, cum3, cum_t, rate_t, after, db_out, dc_out, row_out, col_out, mix, scores):
    step = pl.program_id(0)

    @pl.when(step == 0)
    def _():
        c_hi, c_lo = halves(c[...])
        b_hi, b_lo = halves(b[...])
        scores[...] = mm_nt(c_hi, b_hi) + (mm_nt(c_hi, b_lo) + mm_nt(c_lo, b_hi))
        mix[...] = jnp.zeros_like(mix)
        row_out[...] = jnp.zeros_like(row_out)

    causal = iota((128, 128), 0) >= iota((128, 128), 1)
    left = iota((T, 128), 1) < 64
    per_step = INSIDE_LANES // 64
    pick = iota((384, 128), 0) % 128 == step * per_step + iota((384, 128), 1)
    cols = mm(cum3[...], pick.astype(BF16))
    lane = iota((128, 128), 1)
    sums0 = row_out[0:128, :]
    sums1 = row_out[128:256, :]
    zero = jnp.zeros((), BF16)
    for j in range(per_step):
        head = step * per_step + j
        pair = slice(128 * (j // 2), 128 * (j // 2) + 128)
        v_pair = v[:, pair]
        g_pair = g[:, pair]
        g_head = jnp.where(left if j % 2 == 0 else ~left, g_pair, zero)
        cum_row = cum_t[j : j + 1, :]
        rate_row = rate_t[j : j + 1, :]

        def block(t0, s0):
            t = slice(t0, t0 + 128)
            s = slice(s0, s0 + 128)
            gap = cols[t, j : j + 1] - cum_row[:, s]
            if t0 == s0:
                gap = jnp.where(causal, gap, -1e30)
            part = jnp.exp(gap) * rate_row[:, s] * mm_nt(g_head[t], v_pair[s])
            mix[t, s] += part
            return part * scores[t, s]

        m00 = block(0, 0)
        m10 = block(128, 0)
        m11 = block(128, 128)
        sums0 = jnp.where(lane == head, jnp.sum(m00, axis=1, keepdims=True), sums0)
        sums1 = jnp.where(lane == head, jnp.sum(m10 + m11, axis=1, keepdims=True), sums1)
        col_out[j : j + 1, 0:128] = jnp.sum(m00 + m10, axis=0, keepdims=True)
        col_out[j : j + 1, 128:256] = jnp.sum(m11, axis=0, keepdims=True)
    row_out[0:128, :] = sums0
    row_out[128:256, :] = sums1

    @pl.when(step == pl.num_programs(0) - 1)
    def _():
        m_hi, m_lo = halves(mix[...])
        b_hi, b_lo = halves(b[...])
        c_hi, c_lo = halves(c[...])
        dc_out[...] = mm(m_hi, b_hi) + (mm(m_hi, b_lo) + mm(m_lo, b_hi))
        db_out[...] = mm_tn(m_hi, c_hi) + (mm_tn(m_hi, c_lo) + mm_tn(m_lo, c_hi))


def inside(v, g, b, c, cum3, cum_t, rate_t, after):
    lanes = pl.BlockSpec((T, INSIDE_LANES), lambda i: (0, i))
    some = pl.BlockSpec((INSIDE_LANES // 64, T), lambda i: (i, 0))
    shape = jax.ShapeDtypeStruct
    outs = (shape((T, N), F32), shape((T, N), F32), shape((T, 128), F32), shape((128, T), F32))
    return pl.pallas_call(
        inside_kernel,
        grid=(W // INSIDE_LANES,),
        in_specs=[lanes, lanes, whole((T, N)), whole((T, N)), whole((T, 384)), some, some, pl.BlockSpec(memory_space=pl.ANY)],
        out_specs=[whole((T, N)), whole((T, N)), whole((T, 128)), some],
        out_shape=outs,
        scratch_shapes=[pltpu.VMEM((T, T), F32), pltpu.VMEM((T, T), F32)],
        compiler_params=params("arbitrary"),
        cost_estimate=pl.CostEstimate(flops=20_000_000_000, transcendentals=4_000_000, bytes_accessed=6_000_000),
        name="inside",
    )(v, g, b, c, cum3, cum_t, rate_t, after)


OUTSIDE_LANES = 512


def outside_kernel(v, g, mine, got, tail, grow, b, c, db_out, dc_out, x_out, z_out, link_out):
    step = pl.program_id(0)

    @pl.when(step == 0)
    def _():
        for ref in (db_out, dc_out, x_out, z_out, link_out):
            ref[...] = jnp.zeros_like(ref)

    def side(pair, rows, state, other, spread, gather):
        weighted = scaled(pair[...], spread, rows)
        s_hi, s_lo = halves(state)
        both = jnp.concatenate([s_hi, s_lo], axis=0)
        w_hi, w_lo = halves(weighted)
        far = mm_nt(w_hi, both)
        o_hi = other[...].astype(BF16)
        reached = mm(jnp.concatenate([o_hi, o_hi], axis=1), both)
        return (
            far[:, 0:N] + far[:, N : 2 * N] + mm_nt(w_lo, s_hi),
            mm((weighted * reached).astype(BF16), gather),
        )

    sums = None
    for lane in range(0, OUTSIDE_LANES, LANES):
        s = slice(lane, lane + LANES)
        first = step * (OUTSIDE_LANES // 64) + lane // 64
        spread = spread_matrix(first, LANES)
        gather = gather_matrix(first, LANES)
        state_in = jnp.concatenate([mine[0:HALF, s], got[0:HALF, s]], axis=0)
        state_back = jnp.concatenate([mine[HALF:N, s], got[HALF:N, s]], axis=0)
        joint = jnp.broadcast_to(jnp.sum(state_in * state_back, axis=0, keepdims=True), (8, LANES))
        j0, j1, j2 = thirds(joint)
        new = (
            *side(grow, g[:, s], state_in, c, spread, gather),
            *side(tail, v[:, s], state_back, b, spread, gather),
            mm(j0, gather) + (mm(j1, gather) + mm(j2, gather)),
        )
        sums = new if sums is None else tuple(x + y for x, y in zip(sums, new))
    for ref, value in zip((dc_out, x_out, db_out, z_out, link_out), sums):
        ref[...] += value


def outside(v, g, mine, got, tail, grow, b, c):
    lanes = pl.BlockSpec((T, OUTSIDE_LANES), lambda i: (0, i))
    rows = pl.BlockSpec((N, OUTSIDE_LANES), lambda i: (0, i))
    shape = jax.ShapeDtypeStruct
    outs = (
        shape((T, N), F32), shape((T, N), F32), shape((T, 128), F32), shape((T, 128), F32), shape((8, 128), F32),
    )
    return pl.pallas_call(
        outside_kernel,
        grid=(W // OUTSIDE_LANES,),
        in_specs=[lanes, lanes, rows, rows, whole((T, 256)), whole((T, 256)), whole((T, N)), whole((T, N))],
        out_specs=[whole(o.shape) for o in outs],
        out_shape=outs,
        compiler_params=params("arbitrary"),
        name="outside",
    )(v, g, mine, got, tail, grow, b, c)


GRAD_STEPS = 4
GRAD_ROWS = D // GRAD_STEPS
ROWS = D // 32


def grads_kernel(
    core, tok, db_in, dc_in, db_far, dc_far, rows_in, cols_in, x_far, z_far, link, end, heads,
    own, other,
    d_proj, res, head_row,
):
    step = pl.program_id(0)
    which = core[0]

    @pl.when(step == 0)
    def _():
        second = which == 1
        db = db_in[...] + db_far[...]
        dc = dc_in[...] + dc_far[...]
        d_proj[:, 0:N] = jnp.where(second, pltpu.roll(db, HALF, 1), db).astype(BF16)
        d_proj[:, N : 2 * N] = jnp.where(second, pltpu.roll(dc, HALF, 1), dc).astype(BF16)
        z = z_far[...]
        ahead = rows_in[...] + x_far[...]
        behind = jnp.where(iota((T, 128), 1) < HEADS, cols_in[...].T, 0.0) + z
        d0, d1, d2 = thirds(ahead - behind)
        onward = (iota((T, T), 0) <= iota((T, T), 1)).astype(BF16)
        carry = jnp.exp(end[0:1, :]) * link[0:1, :] + jnp.sum(z, axis=0, keepdims=True)
        flux = mm(onward, d0) + (mm(onward, d1) + mm(onward, d2)) + carry
        d_log = jnp.sum(flux * heads[0], axis=0, keepdims=True)
        d_bias = jnp.sum(behind * heads[2] + flux * heads[1], axis=0, keepdims=True)
        head_row[:, 0:128] = jnp.broadcast_to(d_log, (8, 128))
        head_row[:, 128:256] = jnp.broadcast_to(d_bias, (8, 128))

    res[...] = mm_tn(tok[...], d_proj[...])
    for k in range(GRAD_ROWS // (2 * ROWS)):
        own[k, 0:ROWS] = res[pl.ds(2 * ROWS * k + ROWS * which, ROWS), :]
        own[k, ROWS : ROWS + 8] = head_row[...]
        other[k, 0:ROWS] = res[pl.ds(2 * ROWS * k + ROWS * (1 - which), ROWS), :]
        other[k, ROWS : ROWS + 8] = head_row[...]


def grads(core, tok, *parts):
    shape = jax.ShapeDtypeStruct
    pieces = GRAD_ROWS // (2 * ROWS)
    out = pl.BlockSpec((pieces, ROWS + 8, 2 * N), lambda i: (i, 0, 0))
    return pl.pallas_call(
        grads_kernel,
        grid=(GRAD_STEPS,),
        in_specs=[SCALARS, pl.BlockSpec((T, GRAD_ROWS), lambda i: (0, i))] + [whole(p.shape) for p in parts],
        out_specs=[out, out],
        out_shape=[shape((CHIPS, ROWS + 8, 2 * N), F32)] * 2,
        scratch_shapes=[
            pltpu.VMEM((T, 2 * N), BF16), pltpu.VMEM((GRAD_ROWS, 2 * N), F32), pltpu.VMEM((8, 2 * N), F32),
        ],
        compiler_params=params("arbitrary"),
        name="grads",
    )(core, tok, *parts)


def settle_kernel(fire, pieces, last_bc, last_heads, new_bc, new_heads, packed, square, head_square, heads):
    fires = fire[0] > 0
    weight = fire[0].astype(F32)
    total = pieces[0]
    for k in range(1, CHIPS):
        total = total + pieces[k]
    rows = total[0:ROWS]
    heads[...] = jnp.zeros_like(heads)
    heads[0:1, :] = total[ROWS : ROWS + 1, 0:128]
    heads[1:2, :] = total[ROWS : ROWS + 1, 128:256]
    sums = heads[0:2, 0:HEADS]
    last = last_heads[...]
    new_heads[...] = jnp.where(fires, sums, last)
    diff_heads = sums - last
    diff = rows - last_bc[...]
    new_bc[...] = jnp.where(fires, rows, last_bc[...])
    packed[0:ROWS, :] = weight * diff
    packed[ROWS : ROWS + 8, :] = jnp.zeros((8, 2 * N), F32)
    packed[ROWS : ROWS + 2, 0:HEADS] = weight * diff_heads
    lanes = jnp.sum(diff * diff, axis=0, keepdims=True)
    square[...] = jnp.broadcast_to((lanes[:, 0:128] + lanes[:, 128:256])[None], (32, 1, 128))
    head_square[...] = jnp.broadcast_to(jnp.sum(diff_heads * diff_heads, keepdims=True), (8, 128))


def settle(fire, pieces, last_bc, last_heads):
    shape = jax.ShapeDtypeStruct
    vmem = pl.BlockSpec(memory_space=pltpu.VMEM)
    return pl.pallas_call(
        settle_kernel,
        in_specs=[SCALARS, vmem, vmem, vmem],
        out_specs=[vmem] * 5,
        out_shape=[
            shape((ROWS, 2 * N), F32), shape((2, HEADS), F32), shape((ROWS + 8, 2 * N), F32),
            shape((32, 1, 128), F32), shape((8, 128), F32),
        ],
        scratch_shapes=[pltpu.VMEM((8, 128), F32)],
        compiler_params=params(),
        name="settle",
    )(fire, pieces, last_bc, last_heads)


def finish_kernel(replica, p0, p1, p2, p3, squares, head_square, total_bc, total_heads, new_bc, new_heads, trigger):
    me = replica[0]
    fired = None
    for r in range(4):
        far = (me - r) & 3
        part = jnp.where(far < 2, jnp.where(far == 0, p0[...], p1[...]), jnp.where(far == 2, p2[...], p3[...]))
        fired = part if fired is None else fired + part
    new_bc[...] = total_bc[...] + fired[0:ROWS]
    new_heads[...] = total_heads[...] + fired[ROWS : ROWS + 2, 0:HEADS]
    square = jnp.sum(squares[...][:, 0, :], keepdims=True)
    trigger[...] = jnp.sqrt(square + head_square[0:1, 0:1] + 1e-06)


def finish(replica, parts, squares, head_square, total_bc, total_heads):
    shape = jax.ShapeDtypeStruct
    vmem = pl.BlockSpec(memory_space=pltpu.VMEM)
    return pl.pallas_call(
        finish_kernel,
        in_specs=[SCALARS] + [vmem] * 8,
        out_specs=[vmem] * 3,
        out_shape=[shape((ROWS, 2 * N), F32), shape((2, HEADS), F32), shape((1, 1), F32)],
        compiler_params=params(),
        name="finish",
    )(replica, *parts, squares, head_square, total_bc, total_heads)


def all_to_all(x, axis):
    return lax.all_to_all(x, axis, 0, 0, tiled=True)


def local(
    tokens, values, out_grad, w_bc, w_dt, a_log, dt_bias, fire_flags, last_bc, last_heads, total_bc, total_heads
):
    tok, v, g = tokens[0], values[0], out_grad[0]
    core = lax.axis_index("c").astype(jnp.int32).reshape(1)
    replica = lax.axis_index("dp").astype(jnp.int32).reshape(1)
    own, other, b, c, tail, grow, cum3, cum_t, rate_t, heads, end = front(
        core, tok, w_bc, w_dt.T, a_log.reshape(1, HEADS), dt_bias.reshape(1, HEADS), v, g
    )
    end_other = lax.ppermute(end, "c", CORE_SWAP)
    arrived = lax.ppermute(other, "c", CORE_SWAP)
    terms, arrived = chip_terms(core, own, arrived, end, end_other)
    gathered = all_to_all(terms, RING)
    db_in, dc_in, rows_in, cols_in = inside(v, g, b, c, cum3, cum_t, rate_t, terms)
    states = all_to_all(scan_chips(gathered, rows_in), RING)
    got = lax.ppermute(core_states(True, core, states, own, end, end_other), "c", CORE_SWAP)
    mine = core_states(False, core, states, arrived, end, end_other)
    db_far, dc_far, x_far, z_far, link = outside(v, g, mine, got, tail, grow, b, c)
    rows_own, rows_other = grads(
        core, tok, db_in, dc_in, db_far, dc_far, rows_in, cols_in, x_far, z_far, link, end, heads
    )
    rows = rows_own + lax.ppermute(rows_other, "c", CORE_SWAP)
    new_bc, new_heads, packed, square, head_square = settle(
        fire_flags, all_to_all(rows, RING), last_bc[0], last_heads[0]
    )
    parts = [packed] + [lax.ppermute(packed, "dp", [(r, (r + k) % 4) for r in range(4)]) for k in (1, 2, 3)]
    squares = all_to_all(square, SEQ)
    total_bc, total_heads, trigger = finish(replica, parts, squares, head_square, total_bc, total_heads)
    return total_bc, total_heads, new_bc[None], new_heads[None], trigger.reshape(1)


def solution(mesh):
    split = Mesh(mesh.devices.reshape(mesh.shape["dp"], 4, 4, 2), ("dp",) + SEQ)
    rows = P("dp", SEQ, None)
    in_specs = (
        rows, rows, rows, P(), P(), P(), P(), P("dp"), rows, P("dp", None, None), P(SEQ, None), P(),
    )
    out_specs = (P(SEQ, None), P(), rows, P("dp", None, None), P("dp"))
    return jax.shard_map(local, mesh=split, in_specs=in_specs, out_specs=out_specs, check_vma=False)
```

```python
import functools

import jax
import jax.numpy as jnp
from jax import lax
from jax.experimental import pallas as pl
from jax.experimental.pallas import tpu as pltpu
from jax.sharding import Mesh
from jax.sharding import PartitionSpec as P

F32 = jnp.float32
BF16 = jnp.bfloat16
T = 256
D = 2560
N = 128
HEADS = 80
W = 5120
HALF = 64
CHIPS = 16
SEQ = ("z", "y", "c")
RING = ("z", "y")
CORE_SWAP = [(0, 1), (1, 0)]


def iota(shape, dim):
    return lax.broadcasted_iota(jnp.int32, shape, dim)


def halves(x):
    high = x.astype(BF16)
    return high, (x - high.astype(F32)).astype(BF16)


def thirds(x):
    high = x.astype(BF16)
    rest = x - high.astype(F32)
    mid = rest.astype(BF16)
    return high, mid, (rest - mid.astype(F32)).astype(BF16)


def mm(a, b):
    return jnp.dot(a, b, preferred_element_type=F32)


def mm_nt(a, b):
    return lax.dot_general(a, b, (((1,), (1,)), ((), ())), preferred_element_type=F32)


def mm_tn(a, b):
    return lax.dot_general(a, b, (((0,), (0,)), ((), ())), preferred_element_type=F32)


def spread_matrix(first_head, lanes):
    head = iota((256, lanes), 0) % 128
    return (head == first_head + iota((256, lanes), 1) // 64).astype(BF16)


def gather_matrix(first_head, lanes):
    return (first_head + iota((lanes, 128), 0) // 64 == iota((lanes, 128), 1)).astype(BF16)


def paired(x):
    return jnp.concatenate(halves(x), axis=1)


def whole(shape):
    return pl.BlockSpec(shape, lambda *_: (0,) * len(shape))


SCALARS = pl.BlockSpec(memory_space=pltpu.SMEM)


def params(*semantics):
    return pltpu.CompilerParams(dimension_semantics=semantics, vmem_limit_bytes=20 << 20)


LANES = 256
STEPS = W // LANES


def scaled(pair, spread, rows):
    return mm(pair, spread) * rows.astype(F32)


def three(left, right):
    hi, lo = halves(right)
    wide = mm(left[...], hi)
    return wide[0:N] + (wide[N : 2 * N] + mm(left[0:N], lo))


PARTS = 5
PART_D = D // PARTS
PART_W = W // PARTS
IN_HBM = pl.BlockSpec(memory_space=pltpu.HBM)
IN_VMEM = pl.BlockSpec(memory_space=pltpu.VMEM)


def cut(i, width):
    return slice(i * width, (i + 1) * width)


def rates(wide, row):
    x = wide[...] + row[8:9, :]
    small = jnp.exp(-jnp.abs(x))
    rate = jnp.maximum(x, 0.0) + jnp.log1p(small)
    slope = jnp.where(x >= 0.0, 1.0, small) / (1.0 + small)
    pace = jnp.exp(row[0:1, :])
    return rate, -rate * pace, slope, pace


def running_sum(decay):
    upto = (iota((T, T), 0) >= iota((T, T), 1)).astype(BF16)
    d0, d1, d2 = thirds(decay)
    return mm(upto, d2) + mm(upto, d1) + mm(upto, d0)


def front_kernel(
    core, tok, w_bc, w_dt, a_log, dt_bias, v, g,
    own, other, b_out, c_out, tail_out, grow_out, wide, row, end_out,
    tok_buf, bc_buf, dt_buf, log_buf, bias_buf, v_buf, g_buf, bt, ct,
    tok_sem, bc_sem, dt_sem, row_sem, v_sem, g_sem,
):
    copies = []
    for i in range(PARTS):
        k = cut(i, PART_D)
        copies.append((
            pltpu.make_async_copy(tok.at[:, k], tok_buf.at[i], tok_sem.at[i]),
            pltpu.make_async_copy(w_bc.at[k, :], bc_buf.at[i], bc_sem.at[i]),
            pltpu.make_async_copy(w_dt.at[:, k], dt_buf.at[i], dt_sem.at[i]),
        ))
    small = (
        pltpu.make_async_copy(a_log, log_buf, row_sem.at[0]),
        pltpu.make_async_copy(dt_bias, bias_buf, row_sem.at[1]),
    )
    rows_in = [
        (
            pltpu.make_async_copy(v.at[:, cut(i, PART_W)], v_buf.at[i], v_sem.at[i]),
            pltpu.make_async_copy(g.at[:, cut(i, PART_W)], g_buf.at[i], g_sem.at[i]),
        )
        for i in range(PARTS)
    ]
    for group in copies:
        for copy in group:
            copy.start()
    for copy in small:
        copy.start()
    for group in rows_in:
        for copy in group:
            copy.start()
    row[...] = jnp.zeros_like(row)
    wide[...] = jnp.zeros_like(wide)
    projected = None
    raw_dt = None
    for i in range(PARTS):
        for copy in copies[i]:
            copy.wait()
        u = tok_buf[i]
        part = mm(u, bc_buf[i])
        part_dt = mm_nt(u, dt_buf[i])
        projected = part if i == 0 else projected + part
        raw_dt = part_dt if i == 0 else raw_dt + part_dt
    for copy in small:
        copy.wait()
    row[0:1, 0:HEADS] = log_buf[...]
    row[8:9, 0:HEADS] = bias_buf[...]
    wide[:, 0:HEADS] = raw_dt
    second = core[0] == 1
    b = projected[:, 0:N]
    c = projected[:, N : 2 * N]
    b = jnp.where(second, pltpu.roll(b, HALF, 1), b)
    c = jnp.where(second, pltpu.roll(c, HALF, 1), c)
    b_out[...] = b
    c_out[...] = c
    bt_hi, bt_lo = halves(b.T)
    ct_hi, ct_lo = halves(c.T)
    bt[0:N, :] = bt_hi
    bt[N : 2 * N, :] = bt_lo
    ct[0:N, :] = ct_hi
    ct[N : 2 * N, :] = ct_lo
    rate, decay = rates(wide, row)[0:2]
    cum = running_sum(decay)
    end = cum[T - 1 : T, :]
    tail_out[...] = paired(jnp.exp(end - cum) * rate)
    grow_out[...] = paired(jnp.exp(cum))
    end_out[...] = jnp.broadcast_to(end, (8, 128))

    def add_part(i, _):
        start = pl.multiple_of(i * PART_W, PART_W)
        lanes = pl.ds(start, PART_W)
        pltpu.make_async_copy(v.at[:, lanes], v_buf.at[i], v_sem.at[i]).wait()
        pltpu.make_async_copy(g.at[:, lanes], g_buf.at[i], g_sem.at[i]).wait()
        for lane in range(0, PART_W, LANES):
            s = slice(lane, lane + LANES)
            to = pl.ds(start + lane, LANES)
            spread = spread_matrix(i * (PART_W // 64) + lane // 64, LANES)
            fresh = three(bt, scaled(tail_out[...], spread, v_buf[i, :, s]))
            entry = three(ct, scaled(grow_out[...], spread, g_buf[i, :, s]))
            own[0:HALF, to] = fresh[0:HALF]
            own[HALF:N, to] = entry[0:HALF]
            other[0:HALF, to] = fresh[HALF:N]
            other[HALF:N, to] = entry[HALF:N]
        return 0

    lax.fori_loop(0, PARTS, add_part, 0)


def front(core, tok, w_bc, w_dt, a_log, dt_bias, v, g):
    shape = jax.ShapeDtypeStruct
    vmem = pltpu.VMEM
    dma = pltpu.SemaphoreType.DMA
    outs = (
        shape((N, W), F32), shape((N, W), F32), shape((T, N), F32), shape((T, N), F32),
        shape((T, 256), BF16), shape((T, 256), BF16), shape((T, 128), F32), shape((16, 128), F32), shape((8, 128), F32),
    )
    tok, w_bc, w_dt, a_log, dt_bias, v, g = (
        pltpu.with_memory_space_constraint(x, pltpu.HBM) for x in (tok, w_bc, w_dt, a_log, dt_bias, v, g)
    )
    return pl.pallas_call(
        front_kernel,
        in_specs=[SCALARS] + [IN_HBM] * 7,
        out_specs=[IN_VMEM] * len(outs),
        out_shape=outs,
        scratch_shapes=[
            vmem((PARTS, T, PART_D), BF16), vmem((PARTS, PART_D, 2 * N), BF16), vmem((PARTS, HEADS, PART_D), BF16),
            vmem((1, HEADS), F32), vmem((1, HEADS), F32),
            vmem((PARTS, T, PART_W), BF16), vmem((PARTS, T, PART_W), BF16),
            vmem((2 * N, T), BF16), vmem((2 * N, T), BF16),
            dma((PARTS,)), dma((PARTS,)), dma((PARTS,)), dma((2,)), dma((PARTS,)), dma((PARTS,)),
        ],
        compiler_params=pltpu.CompilerParams(vmem_limit_bytes=28 << 20),
        name="front",
    )(core, tok, w_bc, w_dt, a_log, dt_bias, v, g)


def chip_kernel(core, own, arrived, end, end_other, out):
    second = core[0] == 1
    mine = jnp.exp(end[...])
    theirs = jnp.exp(end_other[...])
    one = jnp.ones_like(mine)
    weights = jnp.concatenate(
        [
            jnp.where(second, one, theirs),
            jnp.where(second, mine, one),
            jnp.where(second, theirs, one),
            jnp.where(second, one, mine),
        ],
        axis=0,
    )
    weights = paired(weights)
    upper = iota((8, 512), 0) < 4
    for lane in range(0, W, 512):
        s = slice(lane, lane + 512)
        scale = mm(weights, spread_matrix(lane // 64, 512))
        for k in range(8):
            r = slice(8 * k, 8 * k + 8)
            q = slice(HALF + 8 * k, HALF + 8 * k + 8)
            fwd = scale[0:8] * own[r, s] + scale[8:16] * arrived[r, s]
            bwd = scale[16:24] * own[q, s] + scale[24:32] * arrived[q, s]
            out[2 * k, :, s] = jnp.where(upper, fwd, pltpu.roll(bwd, 4, 0))
            out[2 * k + 1, :, s] = jnp.where(upper, pltpu.roll(fwd, 4, 0), bwd)
    total = end[...] + end_other[...]
    for k in range(CHIPS):
        out[k, :, W : W + 128] = total


def chip_terms(core, own, arrived, end, end_other):
    return pl.pallas_call(
        chip_kernel,
        in_specs=[SCALARS] + [pl.BlockSpec(memory_space=pltpu.VMEM)] * 4,
        out_specs=pl.BlockSpec(memory_space=pltpu.VMEM),
        out_shape=jax.ShapeDtypeStruct((CHIPS, 8, W + 128), F32),
        compiler_params=params(),
        name="chip_terms",
    )(core, own, arrived, end, end_other)


SCAN_LANES = 1024


def scan_kernel(terms, ends, out):
    width = SCAN_LANES
    decays = paired(jnp.exp(ends[...].reshape(CHIPS * 8, 128)))
    first = pl.program_id(0) * (width // 64)
    upper = iota((8, 512), 0) < 4
    for lane in range(0, width, 512):
        s = slice(lane, lane + 512)
        decay = mm(decays, spread_matrix(first + lane // 64, 512))
        state = jnp.zeros((8, 512), F32)
        for k in range(CHIPS):
            m = CHIPS - 1 - k
            out[k, 0:4, s] = state[0:4]
            out[m, 4:8, s] = state[4:8]
            here = jnp.where(upper, terms[k, :, s], terms[m, :, s])
            rate = jnp.where(upper, decay[8 * k : 8 * k + 8], decay[8 * m : 8 * m + 8])
            state = rate * state + here


def scan_chips(terms):
    return pl.pallas_call(
        scan_kernel,
        grid=(W // SCAN_LANES,),
        in_specs=[
            pl.BlockSpec((CHIPS, 8, SCAN_LANES), lambda i: (0, 0, i)),
            pl.BlockSpec((CHIPS, 8, 128), lambda i: (0, 0, W // 128)),
        ],
        out_specs=pl.BlockSpec((CHIPS, 8, SCAN_LANES), lambda i: (0, 0, i)),
        out_shape=pltpu.HBM((CHIPS, 8, W), F32),
        compiler_params=params("arbitrary"),
        name="scan_chips",
    )(terms, terms)


def core_kernel(
    sending, core, states, part, end, end_other, after, fwd_out, bwd_out, states_buf, part_buf, states_sem, part_sem
):
    lanes = [cut(i, PART_W) for i in range(PARTS)]
    row = pl.multiple_of(HALF * (core[0] if sending else 1 - core[0]), HALF)
    copies = [
        (
            pltpu.make_async_copy(states.at[:, :, s], states_buf.at[i], states_sem.at[i]),
            pltpu.make_async_copy(part.at[pl.ds(row, HALF), s], part_buf.at[i], part_sem.at[i]),
        )
        for i, s in enumerate(lanes)
    ]
    for group in copies:
        for copy in group:
            copy.start()
    forward = (core[0] == 0) == sending
    decay = jnp.exp(jnp.where(sending, end[...], end_other[...]))
    one = jnp.ones_like(decay)
    zero = jnp.zeros_like(decay)
    weights = paired(
        jnp.concatenate(
            [
                jnp.where(forward, decay, one),
                jnp.where(forward, one, zero),
                jnp.where(forward, one, decay),
                jnp.where(forward, zero, one),
            ],
            axis=0,
        )
    )
    upper = iota((8, 512), 0) < 4
    for i in range(PARTS):
        for copy in copies[i]:
            copy.wait()
        for lane in range(0, PART_W, 512):
            s = slice(lane, lane + 512)
            to = slice(i * PART_W + lane, i * PART_W + lane + 512)
            w = mm(weights, spread_matrix((i * PART_W + lane) // 64, 512))
            for k in range(8):
                r = slice(8 * k, 8 * k + 8)
                even = states_buf[i, 2 * k, :, s]
                odd = states_buf[i, 2 * k + 1, :, s]
                fwd = jnp.where(upper, even, pltpu.roll(odd, 4, 0))
                bwd = jnp.where(upper, pltpu.roll(even, 4, 0), odd)
                extra = part_buf[i, r, s]
                fwd_out[r, to] = w[0:8] * fwd + w[8:16] * extra
                bwd_out[r, to] = w[16:24] * bwd + w[24:32] * extra


def core_states(sending, core, states, part, end, end_other, after):
    states, part = (pltpu.with_memory_space_constraint(x, pltpu.HBM) for x in (states, part))
    dma = pltpu.SemaphoreType.DMA
    return pl.pallas_call(
        functools.partial(core_kernel, sending),
        in_specs=[SCALARS, IN_HBM, IN_HBM, IN_VMEM, IN_VMEM, pl.BlockSpec(memory_space=pl.ANY)],
        out_specs=[IN_VMEM] * 2,
        out_shape=[jax.ShapeDtypeStruct((HALF, W), F32)] * 2,
        scratch_shapes=[
            pltpu.VMEM((PARTS, CHIPS, 8, PART_W), F32), pltpu.VMEM((PARTS, HALF, PART_W), F32),
            dma((PARTS,)), dma((PARTS,)),
        ],
        compiler_params=params(),
        cost_estimate=pl.CostEstimate(flops=2_000_000_000, transcendentals=0, bytes_accessed=8_000_000),
        name="sent_states" if sending else "own_states",
    )(core, states, part, end, end_other, after)


INSIDE_LANES = 512


def inside_kernel(
    v, g, b, c, wide, row, tail, grow, after,
    db_out, dc_out, row_out, col_out, heads_out, v_hi, v_lo, g_hi, g_lo,
    mix, scores, cum3, cum_rows, rate_rows,
):
    step = pl.program_id(0)

    @pl.when(step == 0)
    def _():
        c_hi, c_lo = halves(c[...])
        b_hi, b_lo = halves(b[...])
        scores[...] = mm_nt(c_hi, b_hi) + (mm_nt(c_hi, b_lo) + mm_nt(c_lo, b_hi))
        mix[...] = jnp.zeros_like(mix)
        row_out[...] = jnp.zeros_like(row_out)
        rate, decay, slope, pace = rates(wide, row)
        cum = running_sum(decay)
        for k, part in enumerate(thirds(cum)):
            cum3[:, 128 * k : 128 * k + 128] = part
        cum_rows[...] = cum.T
        rate_rows[...] = rate.T
        heads_out[0] = decay
        heads_out[1] = -pace * slope
        heads_out[2] = jnp.where(rate > 0.0, slope / rate, 0.0)

    causal = iota((128, 128), 0) >= iota((128, 128), 1)
    left = iota((T, 128), 1) < 64
    per_step = INSIDE_LANES // 64
    pick = iota((384, 128), 0) % 128 == step * per_step + iota((384, 128), 1)
    cols = mm(cum3[...], pick.astype(BF16))
    some = pl.ds(pl.multiple_of(step * per_step, per_step), per_step)
    cum_t = cum_rows[some, :]
    rate_t = rate_rows[some, :]
    lane = iota((128, 128), 1)
    sums0 = row_out[0:128, :]
    sums1 = row_out[128:256, :]
    zero = jnp.zeros((), BF16)
    for j in range(per_step):
        head = step * per_step + j
        pair = slice(128 * (j // 2), 128 * (j // 2) + 128)
        v_pair = v[:, pair]
        g_pair = g[:, pair]
        g_head = jnp.where(left if j % 2 == 0 else ~left, g_pair, zero)
        cum_row = cum_t[j : j + 1, :]
        rate_row = rate_t[j : j + 1, :]

        def block(t0, s0):
            t = slice(t0, t0 + 128)
            s = slice(s0, s0 + 128)
            gap = cols[t, j : j + 1] - cum_row[:, s]
            if t0 == s0:
                gap = jnp.where(causal, gap, -1e30)
            part = jnp.exp(gap) * rate_row[:, s] * mm_nt(g_head[t], v_pair[s])
            mix[t, s] += part
            return part * scores[t, s]

        m00 = block(0, 0)
        m10 = block(128, 0)
        m11 = block(128, 128)
        sums0 = jnp.where(lane == head, jnp.sum(m00, axis=1, keepdims=True), sums0)
        sums1 = jnp.where(lane == head, jnp.sum(m10 + m11, axis=1, keepdims=True), sums1)
        col_out[j : j + 1, 0:128] = jnp.sum(m00 + m10, axis=0, keepdims=True)
        col_out[j : j + 1, 128:256] = jnp.sum(m11, axis=0, keepdims=True)
    row_out[0:128, :] = sums0
    row_out[128:256, :] = sums1
    for part in range(0, INSIDE_LANES, LANES):
        s = slice(part, part + LANES)
        spread = spread_matrix(step * per_step + part // 64, LANES)
        v_hi[:, s], v_lo[:, s] = halves(scaled(tail[...], spread, v[:, s]))
        g_hi[:, s], g_lo[:, s] = halves(scaled(grow[...], spread, g[:, s]))

    @pl.when(step == pl.num_programs(0) - 1)
    def _():
        m_hi, m_lo = halves(mix[...])
        b_hi, b_lo = halves(b[...])
        c_hi, c_lo = halves(c[...])
        dc_out[...] = mm(m_hi, b_hi) + (mm(m_hi, b_lo) + mm(m_lo, b_hi))
        db_out[...] = mm_tn(m_hi, c_hi) + (mm_tn(m_hi, c_lo) + mm_tn(m_lo, c_hi))


def inside(v, g, b, c, wide, row, tail, grow, after):
    lanes = pl.BlockSpec((T, INSIDE_LANES), lambda i: (0, i))
    some = pl.BlockSpec((INSIDE_LANES // 64, T), lambda i: (i, 0))
    shape = jax.ShapeDtypeStruct
    outs = (shape((T, N), F32), shape((T, N), F32), shape((T, 128), F32), shape((128, T), F32))
    outs += (shape((3, T, 128), F32),)
    outs += (pltpu.HBM((T, W), BF16),) * 4
    return pl.pallas_call(
        inside_kernel,
        grid=(W // INSIDE_LANES,),
        in_specs=[
            lanes, lanes, whole((T, N)), whole((T, N)), whole((T, 128)), whole((16, 128)),
            whole((T, 256)), whole((T, 256)), pl.BlockSpec(memory_space=pl.ANY),
        ],
        out_specs=[whole((T, N)), whole((T, N)), whole((T, 128)), some, whole((3, T, 128))] + [lanes] * 4,
        out_shape=outs,
        scratch_shapes=[
            pltpu.VMEM((T, T), F32), pltpu.VMEM((T, T), F32), pltpu.VMEM((T, 384), BF16),
            pltpu.VMEM((128, T), F32), pltpu.VMEM((128, T), F32),
        ],
        compiler_params=params("arbitrary"),
        cost_estimate=pl.CostEstimate(flops=20_000_000_000, transcendentals=4_000_000, bytes_accessed=6_000_000),
        name="inside",
    )(v, g, b, c, wide, row, tail, grow, after)


OUTSIDE_LANES = 1024


def outside_kernel(linked, *refs):
    if linked:
        rows_hi, rows_lo, mine, got, other, mine_in, got_in, d_out, sum_out, link_out = refs
    else:
        rows_hi, rows_lo, mine, got, other, d_out, sum_out = refs
    step = pl.program_id(0)

    @pl.when(step == 0)
    def _():
        for ref in (d_out, sum_out) + ((link_out,) if linked else ()):
            ref[...] = jnp.zeros_like(ref)

    gather = gather_matrix(step * (OUTSIDE_LANES // 64), OUTSIDE_LANES)
    state = jnp.concatenate([mine[...], got[...]], axis=0)
    s_hi, s_lo = halves(state)
    both = jnp.concatenate([s_hi, s_lo], axis=0)
    far = mm_nt(rows_hi[...], both)
    d_out[...] += far[:, 0:N] + far[:, N : 2 * N] + mm_nt(rows_lo[...], s_hi)
    o_hi = other[...].astype(BF16)
    o_two = jnp.concatenate([o_hi, o_hi], axis=1)
    total = sum_out[...]
    for lane in range(0, OUTSIDE_LANES, LANES):
        s = slice(lane, lane + LANES)
        term = (rows_hi[:, s].astype(F32) * mm(o_two, both[:, s])).astype(BF16)
        total = total + mm(term, gather[s])
    sum_out[...] = total
    if linked:
        state_in = jnp.concatenate([mine_in[...], got_in[...]], axis=0)
        joint = jnp.broadcast_to(jnp.sum(state_in * state, axis=0, keepdims=True), (8, OUTSIDE_LANES))
        j0, j1, j2 = thirds(joint)
        link_out[...] += mm(j0, gather) + (mm(j1, gather) + mm(j2, gather))


def outside(rows_hi, rows_lo, mine, got, other, *states_in):
    linked = len(states_in) > 0
    rows_hi, rows_lo = (pltpu.with_memory_space_constraint(x, pltpu.HBM) for x in (rows_hi, rows_lo))
    lanes = pl.BlockSpec((T, OUTSIDE_LANES), lambda i: (0, i))
    rows = pl.BlockSpec((HALF, OUTSIDE_LANES), lambda i: (0, i))
    shape = jax.ShapeDtypeStruct
    outs = (shape((T, N), F32), shape((T, 128), F32)) + ((shape((8, 128), F32),) if linked else ())
    return pl.pallas_call(
        functools.partial(outside_kernel, linked),
        grid=(W // OUTSIDE_LANES,),
        in_specs=[lanes, lanes, rows, rows, whole((T, N))] + [rows] * len(states_in),
        out_specs=[whole(o.shape) for o in outs],
        out_shape=outs,
        compiler_params=params("arbitrary"),
        cost_estimate=pl.CostEstimate(flops=6_000_000_000, transcendentals=0, bytes_accessed=8_000_000),
        name="outside_back" if linked else "outside_in",
    )(rows_hi, rows_lo, mine, got, other, *states_in)


GRAD_STEPS = 4
GRAD_ROWS = D // GRAD_STEPS
ROWS = D // 32


def grads_kernel(
    core, tok, db_in, dc_in, db_far, dc_far, rows_in, cols_in, x_far, z_far, link, end, heads,
    own, other,
    d_proj, res, head_row,
):
    step = pl.program_id(0)
    which = core[0]

    @pl.when(step == 0)
    def _():
        second = which == 1
        db = db_in[...] + db_far[...]
        dc = dc_in[...] + dc_far[...]
        d_proj[:, 0:N] = jnp.where(second, pltpu.roll(db, HALF, 1), db).astype(BF16)
        d_proj[:, N : 2 * N] = jnp.where(second, pltpu.roll(dc, HALF, 1), dc).astype(BF16)
        z = z_far[...]
        ahead = rows_in[...] + x_far[...]
        behind = jnp.where(iota((T, 128), 1) < HEADS, cols_in[...].T, 0.0) + z
        d0, d1, d2 = thirds(ahead - behind)
        onward = (iota((T, T), 0) <= iota((T, T), 1)).astype(BF16)
        carry = jnp.exp(end[0:1, :]) * link[0:1, :] + jnp.sum(z, axis=0, keepdims=True)
        flux = mm(onward, d0) + (mm(onward, d1) + mm(onward, d2)) + carry
        d_log = jnp.sum(flux * heads[0], axis=0, keepdims=True)
        d_bias = jnp.sum(behind * heads[2] + flux * heads[1], axis=0, keepdims=True)
        head_row[:, 0:128] = jnp.broadcast_to(d_log, (8, 128))
        head_row[:, 128:256] = jnp.broadcast_to(d_bias, (8, 128))

    res[...] = mm_tn(tok[...], d_proj[...])
    for k in range(GRAD_ROWS // (2 * ROWS)):
        own[k, 0:ROWS] = res[pl.ds(2 * ROWS * k + ROWS * which, ROWS), :]
        own[k, ROWS : ROWS + 8] = head_row[...]
        other[k, 0:ROWS] = res[pl.ds(2 * ROWS * k + ROWS * (1 - which), ROWS), :]
        other[k, ROWS : ROWS + 8] = head_row[...]


def grads(core, tok, *parts):
    shape = jax.ShapeDtypeStruct
    pieces = GRAD_ROWS // (2 * ROWS)
    out = pl.BlockSpec((pieces, ROWS + 8, 2 * N), lambda i: (i, 0, 0))
    return pl.pallas_call(
        grads_kernel,
        grid=(GRAD_STEPS,),
        in_specs=[SCALARS, pl.BlockSpec((T, GRAD_ROWS), lambda i: (0, i))] + [whole(p.shape) for p in parts],
        out_specs=[out, out],
        out_shape=[shape((CHIPS, ROWS + 8, 2 * N), F32)] * 2,
        scratch_shapes=[
            pltpu.VMEM((T, 2 * N), BF16), pltpu.VMEM((GRAD_ROWS, 2 * N), F32), pltpu.VMEM((8, 2 * N), F32),
        ],
        compiler_params=params("arbitrary"),
        name="grads",
    )(core, tok, *parts)


def settle_kernel(fire, pieces, last_bc, last_heads, new_bc, new_heads, packed, square, head_square, heads):
    fires = fire[0] > 0
    weight = fire[0].astype(F32)
    total = pieces[0]
    for k in range(1, CHIPS):
        total = total + pieces[k]
    rows = total[0:ROWS]
    heads[...] = jnp.zeros_like(heads)
    heads[0:1, :] = total[ROWS : ROWS + 1, 0:128]
    heads[1:2, :] = total[ROWS : ROWS + 1, 128:256]
    sums = heads[0:2, 0:HEADS]
    last = last_heads[...]
    new_heads[...] = jnp.where(fires, sums, last)
    diff_heads = sums - last
    diff = rows - last_bc[...]
    new_bc[...] = jnp.where(fires, rows, last_bc[...])
    packed[0:ROWS, :] = weight * diff
    packed[ROWS : ROWS + 8, :] = jnp.zeros((8, 2 * N), F32)
    packed[ROWS : ROWS + 2, 0:HEADS] = weight * diff_heads
    lanes = jnp.sum(diff * diff, axis=0, keepdims=True)
    square[...] = jnp.broadcast_to(lanes[:, 0:128] + lanes[:, 128:256], (8, 128))
    head_square[...] = jnp.broadcast_to(jnp.sum(diff_heads * diff_heads, keepdims=True), (8, 128))


def settle(fire, pieces, last_bc, last_heads):
    shape = jax.ShapeDtypeStruct
    vmem = pl.BlockSpec(memory_space=pltpu.VMEM)
    return pl.pallas_call(
        settle_kernel,
        in_specs=[SCALARS, vmem, vmem, vmem],
        out_specs=[vmem] * 5,
        out_shape=[
            shape((ROWS, 2 * N), F32), shape((2, HEADS), F32), shape((ROWS + 8, 2 * N), F32),
            shape((8, 128), F32), shape((8, 128), F32),
        ],
        scratch_shapes=[pltpu.VMEM((8, 128), F32)],
        compiler_params=params(),
        name="settle",
    )(fire, pieces, last_bc, last_heads)


def ring_sum(x0, x1, x2, x3):
    return (x0 + x2) + (x1 + x3)


def finish_kernel(
    p0, p1, p2, p3, s0, s1, s2, s3, head_square, total_bc, total_heads, new_bc, new_heads, trigger
):
    fired = ring_sum(p0[...], p1[...], p2[...], p3[...])
    new_bc[...] = total_bc[...] + fired[0:ROWS]
    new_heads[...] = total_heads[...] + fired[ROWS : ROWS + 2, 0:HEADS]
    square = jnp.sum(ring_sum(s0[...], s1[...], s2[...], s3[...])[0:1], keepdims=True)
    trigger[...] = jnp.sqrt(square + head_square[0:1, 0:1] + 1e-06)


def finish(parts, squares, head_square, total_bc, total_heads):
    shape = jax.ShapeDtypeStruct
    vmem = pl.BlockSpec(memory_space=pltpu.VMEM)
    return pl.pallas_call(
        finish_kernel,
        in_specs=[vmem] * 11,
        out_specs=[vmem] * 3,
        out_shape=[shape((ROWS, 2 * N), F32), shape((2, HEADS), F32), shape((1, 1), F32)],
        compiler_params=params(),
        name="finish",
    )(*parts, *squares, head_square, total_bc, total_heads)


def on_ring(x, axis):
    return [x] + [lax.ppermute(x, axis, [(r, (r + k) % 4) for r in range(4)]) for k in (1, 2, 3)]


def all_to_all(x, axis):
    return lax.all_to_all(x, axis, 0, 0, tiled=True)


def local(
    tokens, values, out_grad, w_bc, w_dt, a_log, dt_bias, fire_flags, last_bc, last_heads, total_bc, total_heads
):
    tok, v, g = tokens[0], values[0], out_grad[0]
    core = lax.axis_index("c").astype(jnp.int32).reshape(1)
    own, other, b, c, tail, grow, wide, row, end = front(
        core, tok, w_bc, w_dt.T, a_log.reshape(1, HEADS), dt_bias.reshape(1, HEADS), v, g
    )
    end_other = lax.ppermute(end, "c", CORE_SWAP)
    arrived = lax.ppermute(other, "c", CORE_SWAP)
    terms = chip_terms(core, own, arrived, end, end_other)
    before = scan_chips(all_to_all(terms, RING))
    states = all_to_all(before, RING)
    db_in, dc_in, rows_in, cols_in, heads, v_hi, v_lo, g_hi, g_lo = inside(
        v, g, b, c, wide, row, tail, grow, before
    )
    sent_in, sent_back = core_states(True, core, states, own, end, end_other, rows_in)
    got_in = lax.ppermute(sent_in, "c", CORE_SWAP)
    got_back = lax.ppermute(sent_back, "c", CORE_SWAP)
    mine_in, mine_back = core_states(False, core, states, arrived, end, end_other, rows_in)
    dc_far, x_far = outside(g_hi, g_lo, mine_in, got_in, c)
    db_far, z_far, link = outside(v_hi, v_lo, mine_back, got_back, b, mine_in, got_in)
    rows_own, rows_other = grads(
        core, tok, db_in, dc_in, db_far, dc_far, rows_in, cols_in, x_far, z_far, link, end, heads
    )
    rows = rows_own + lax.ppermute(rows_other, "c", CORE_SWAP)
    new_bc, new_heads, packed, square, head_square = settle(
        fire_flags, all_to_all(rows, RING), last_bc[0], last_heads[0]
    )
    on_chip = square + lax.ppermute(square, "c", CORE_SWAP)
    squares = on_ring(ring_sum(*on_ring(on_chip, "y")), "z")
    total_bc, total_heads, trigger = finish(on_ring(packed, "dp"), squares, head_square, total_bc, total_heads)
    return total_bc, total_heads, new_bc[None], new_heads[None], trigger.reshape(1)


def solution(mesh):
    split = Mesh(mesh.devices.reshape(mesh.shape["dp"], 4, 4, 2), ("dp",) + SEQ)
    rows = P("dp", SEQ, None)
    in_specs = (
        rows, rows, rows, P(), P(), P(), P(), P("dp"), rows, P("dp", None, None), P(SEQ, None), P(),
    )
    out_specs = (P(SEQ, None), P(), rows, P("dp", None, None), P("dp"))
    return jax.shard_map(local, mesh=split, in_specs=in_specs, out_specs=out_specs, check_vma=False)
```

```python
import functools

import jax
import jax.numpy as jnp
from jax import lax
from jax.experimental import pallas as pl
from jax.experimental.pallas import tpu as pltpu
from jax.sharding import Mesh
from jax.sharding import PartitionSpec as P

F32 = jnp.float32
BF16 = jnp.bfloat16
T = 256
D = 2560
N = 128
HEADS = 80
W = 5120
HALF = 64
CHIPS = 16
SEQ = ("z", "y", "c")
RING = ("z", "y")
CORE_SWAP = [(0, 1), (1, 0)]


def iota(shape, dim):
    return lax.broadcasted_iota(jnp.int32, shape, dim)


def halves(x):
    high = x.astype(BF16)
    return high, (x - high.astype(F32)).astype(BF16)


def thirds(x):
    high = x.astype(BF16)
    rest = x - high.astype(F32)
    mid = rest.astype(BF16)
    return high, mid, (rest - mid.astype(F32)).astype(BF16)


def mm(a, b):
    return jnp.dot(a, b, preferred_element_type=F32)


def mm_nt(a, b):
    return lax.dot_general(a, b, (((1,), (1,)), ((), ())), preferred_element_type=F32)


def mm_tn(a, b):
    return lax.dot_general(a, b, (((0,), (0,)), ((), ())), preferred_element_type=F32)


def spread_matrix(first_head, lanes):
    head = iota((256, lanes), 0) % 128
    return (head == first_head + iota((256, lanes), 1) // 64).astype(BF16)


def gather_matrix(first_head, lanes):
    return (first_head + iota((lanes, 128), 0) // 64 == iota((lanes, 128), 1)).astype(BF16)


def paired(x):
    return jnp.concatenate(halves(x), axis=1)


def whole(shape):
    return pl.BlockSpec(shape, lambda *_: (0,) * len(shape))


SCALARS = pl.BlockSpec(memory_space=pltpu.SMEM)


def params(*semantics):
    return pltpu.CompilerParams(dimension_semantics=semantics, vmem_limit_bytes=20 << 20)


LANES = 256
STEPS = W // LANES


def scaled(pair, spread, rows):
    return mm(pair, spread) * rows.astype(F32)


def three(left, right):
    hi, lo = halves(right)
    wide = mm(left[...], hi)
    return wide[0:N] + (wide[N : 2 * N] + mm(left[0:N], lo))


PARTS = 5
PART_D = D // PARTS
PART_W = W // PARTS
IN_HBM = pl.BlockSpec(memory_space=pltpu.HBM)
IN_VMEM = pl.BlockSpec(memory_space=pltpu.VMEM)


def cut(i, width):
    return slice(i * width, (i + 1) * width)


def rates(wide, row):
    x = wide[...] + row[8:9, :]
    small = jnp.exp(-jnp.abs(x))
    rate = jnp.maximum(x, 0.0) + jnp.log1p(small)
    slope = jnp.where(x >= 0.0, 1.0, small) / (1.0 + small)
    pace = jnp.exp(row[0:1, :])
    return rate, -rate * pace, slope, pace


def running_sum(decay):
    upto = (iota((T, T), 0) >= iota((T, T), 1)).astype(BF16)
    d0, d1, d2 = thirds(decay)
    return mm(upto, d2) + mm(upto, d1) + mm(upto, d0)


def front_kernel(
    core, tok, w_bc, w_dt, a_log, dt_bias, v, g,
    own, other, b_out, c_out, tail_out, grow_out, wide, row, end_out,
    tok_buf, bc_buf, dt_buf, log_buf, bias_buf, v_buf, g_buf, bt, ct, hi_buf, lo_buf,
    tok_sem, bc_sem, dt_sem, row_sem, v_sem, g_sem,
):
    copies = []
    for i in range(PARTS):
        k = cut(i, PART_D)
        copies.append((
            pltpu.make_async_copy(tok.at[:, k], tok_buf.at[i], tok_sem.at[i]),
            pltpu.make_async_copy(w_bc.at[k, :], bc_buf.at[i], bc_sem.at[i]),
            pltpu.make_async_copy(w_dt.at[:, k], dt_buf.at[i], dt_sem.at[i]),
        ))
    small = (
        pltpu.make_async_copy(a_log, log_buf, row_sem.at[0]),
        pltpu.make_async_copy(dt_bias, bias_buf, row_sem.at[1]),
    )
    rows_in = [
        (
            pltpu.make_async_copy(v.at[:, cut(i, PART_W)], v_buf.at[i], v_sem.at[i]),
            pltpu.make_async_copy(g.at[:, cut(i, PART_W)], g_buf.at[i], g_sem.at[i]),
        )
        for i in range(PARTS)
    ]
    for group in copies:
        for copy in group:
            copy.start()
    for copy in small:
        copy.start()
    for group in rows_in:
        for copy in group:
            copy.start()
    row[...] = jnp.zeros_like(row)
    wide[...] = jnp.zeros_like(wide)
    projected = None
    raw_dt = None
    for i in range(PARTS):
        for copy in copies[i]:
            copy.wait()
        u = tok_buf[i]
        part = mm(u, bc_buf[i])
        part_dt = mm_nt(u, dt_buf[i])
        projected = part if i == 0 else projected + part
        raw_dt = part_dt if i == 0 else raw_dt + part_dt
    for copy in small:
        copy.wait()
    row[0:1, 0:HEADS] = log_buf[...]
    row[8:9, 0:HEADS] = bias_buf[...]
    wide[:, 0:HEADS] = raw_dt
    second = core[0] == 1
    b = projected[:, 0:N]
    c = projected[:, N : 2 * N]
    b = jnp.where(second, pltpu.roll(b, HALF, 1), b)
    c = jnp.where(second, pltpu.roll(c, HALF, 1), c)
    b_out[...] = b
    c_out[...] = c
    bt_hi, bt_lo = halves(b.T)
    ct_hi, ct_lo = halves(c.T)
    bt[0:N, :] = bt_hi
    bt[N : 2 * N, :] = bt_lo
    ct[0:N, :] = ct_hi
    ct[N : 2 * N, :] = ct_lo
    rate, decay = rates(wide, row)[0:2]
    cum = running_sum(decay)
    end = cum[T - 1 : T, :]
    tail_out[...] = paired(jnp.exp(end - cum) * rate)
    grow_out[...] = paired(jnp.exp(cum))
    end_out[...] = jnp.broadcast_to(end, (8, 128))

    def add_part(i, _):
        start = pl.multiple_of(i * PART_W, PART_W)
        lanes = pl.ds(start, PART_W)
        pltpu.make_async_copy(v.at[:, lanes], v_buf.at[i], v_sem.at[i]).wait()
        pltpu.make_async_copy(g.at[:, lanes], g_buf.at[i], g_sem.at[i]).wait()
        for lane in range(0, PART_W, LANES):
            s = slice(lane, lane + LANES)
            spread = spread_matrix(i * (PART_W // 64) + lane // 64, LANES)
            for n, (pair, rows) in enumerate(((tail_out, v_buf), (grow_out, g_buf))):
                hi, lo = halves(scaled(pair[...], spread, rows[i, :, s]))
                hi_buf[n, :, s] = hi
                lo_buf[n, :, s] = lo
        for lane in range(0, PART_W, 2 * LANES):
            s = slice(lane, lane + 2 * LANES)
            to = pl.ds(start + lane, 2 * LANES)
            for n, left in enumerate((bt, ct)):
                hi = hi_buf[n, :, s]
                wide_sum = mm(left[...], hi)
                total = wide_sum[0:N] + (wide_sum[N : 2 * N] + mm(left[0:N], lo_buf[n, :, s]))
                r = slice(HALF * n, HALF * n + HALF)
                own[r, to] = total[0:HALF]
                other[r, to] = total[HALF:N]
        return 0

    lax.fori_loop(0, PARTS, add_part, 0)


def front(core, tok, w_bc, w_dt, a_log, dt_bias, v, g):
    shape = jax.ShapeDtypeStruct
    vmem = pltpu.VMEM
    dma = pltpu.SemaphoreType.DMA
    outs = (
        shape((N, W), F32), shape((N, W), F32), shape((T, N), F32), shape((T, N), F32),
        shape((T, 256), BF16), shape((T, 256), BF16), shape((T, 128), F32), shape((16, 128), F32), shape((8, 128), F32),
    )
    tok, w_bc, w_dt, a_log, dt_bias, v, g = (
        pltpu.with_memory_space_constraint(x, pltpu.HBM) for x in (tok, w_bc, w_dt, a_log, dt_bias, v, g)
    )
    return pl.pallas_call(
        front_kernel,
        in_specs=[SCALARS] + [IN_HBM] * 7,
        out_specs=[IN_VMEM] * len(outs),
        out_shape=outs,
        scratch_shapes=[
            vmem((PARTS, T, PART_D), BF16), vmem((PARTS, PART_D, 2 * N), BF16), vmem((PARTS, HEADS, PART_D), BF16),
            vmem((1, HEADS), F32), vmem((1, HEADS), F32),
            vmem((PARTS, T, PART_W), BF16), vmem((PARTS, T, PART_W), BF16),
            vmem((2 * N, T), BF16), vmem((2 * N, T), BF16), vmem((2, T, PART_W), BF16), vmem((2, T, PART_W), BF16),
            dma((PARTS,)), dma((PARTS,)), dma((PARTS,)), dma((2,)), dma((PARTS,)), dma((PARTS,)),
        ],
        compiler_params=pltpu.CompilerParams(vmem_limit_bytes=28 << 20),
        name="front",
    )(core, tok, w_bc, w_dt, a_log, dt_bias, v, g)


def chip_kernel(core, own, arrived, end, end_other, out):
    second = core[0] == 1
    mine = jnp.exp(end[...])
    theirs = jnp.exp(end_other[...])
    one = jnp.ones_like(mine)
    weights = jnp.concatenate(
        [
            jnp.where(second, one, theirs),
            jnp.where(second, mine, one),
            jnp.where(second, theirs, one),
            jnp.where(second, one, mine),
        ],
        axis=0,
    )
    weights = paired(weights)
    upper = iota((8, 512), 0) < 4
    for lane in range(0, W, 512):
        s = slice(lane, lane + 512)
        scale = mm(weights, spread_matrix(lane // 64, 512))
        for k in range(8):
            r = slice(8 * k, 8 * k + 8)
            q = slice(HALF + 8 * k, HALF + 8 * k + 8)
            fwd = scale[0:8] * own[r, s] + scale[8:16] * arrived[r, s]
            bwd = scale[16:24] * own[q, s] + scale[24:32] * arrived[q, s]
            out[2 * k, :, s] = jnp.where(upper, fwd, pltpu.roll(bwd, 4, 0))
            out[2 * k + 1, :, s] = jnp.where(upper, pltpu.roll(fwd, 4, 0), bwd)
    total = end[...] + end_other[...]
    for k in range(CHIPS):
        out[k, :, W : W + 128] = total


def chip_terms(core, own, arrived, end, end_other):
    return pl.pallas_call(
        chip_kernel,
        in_specs=[SCALARS] + [pl.BlockSpec(memory_space=pltpu.VMEM)] * 4,
        out_specs=pl.BlockSpec(memory_space=pltpu.VMEM),
        out_shape=jax.ShapeDtypeStruct((CHIPS, 8, W + 128), F32),
        compiler_params=params(),
        name="chip_terms",
    )(core, own, arrived, end, end_other)


def scan_kernel(terms, out, out_buf, out_sem):
    decays = paired(jnp.exp(terms[:, :, W : W + 128].reshape(CHIPS * 8, 128)))
    upper = iota((8, 512), 0) < 4
    copies = []
    for lane in range(0, W, 512):
        s = slice(lane, lane + 512)
        decay = mm(decays, spread_matrix(lane // 64, 512))
        state = jnp.zeros((8, 512), F32)
        for k in range(CHIPS):
            m = CHIPS - 1 - k
            out_buf[k, 0:4, s] = state[0:4]
            out_buf[m, 4:8, s] = state[4:8]
            here = jnp.where(upper, terms[k, :, s], terms[m, :, s])
            rate = jnp.where(upper, decay[8 * k : 8 * k + 8], decay[8 * m : 8 * m + 8])
            state = rate * state + here
        copy = pltpu.make_async_copy(out_buf.at[:, :, s], out.at[:, :, s], out_sem.at[lane // 512])
        copy.start()
        copies.append(copy)
    for copy in copies:
        copy.wait()


def scan_chips(terms):
    return pl.pallas_call(
        scan_kernel,
        in_specs=[IN_VMEM],
        out_specs=IN_HBM,
        out_shape=pltpu.HBM((CHIPS, 8, W), F32),
        scratch_shapes=[pltpu.VMEM((CHIPS, 8, W), F32), pltpu.SemaphoreType.DMA((W // 512,))],
        compiler_params=params(),
        name="scan_chips",
    )(terms)


def core_kernel(
    sending, core, states, part, end, end_other, after, fwd_out, bwd_out, states_buf, part_buf, states_sem, part_sem
):
    lanes = [cut(i, PART_W) for i in range(PARTS)]
    row = pl.multiple_of(HALF * (core[0] if sending else 1 - core[0]), HALF)
    copies = [
        (
            pltpu.make_async_copy(states.at[:, :, s], states_buf.at[i], states_sem.at[i]),
            pltpu.make_async_copy(part.at[pl.ds(row, HALF), s], part_buf.at[i], part_sem.at[i]),
        )
        for i, s in enumerate(lanes)
    ]
    for group in copies:
        for copy in group:
            copy.start()
    forward = (core[0] == 0) == sending
    decay = jnp.exp(jnp.where(sending, end[...], end_other[...]))
    one = jnp.ones_like(decay)
    zero = jnp.zeros_like(decay)
    weights = paired(
        jnp.concatenate(
            [
                jnp.where(forward, decay, one),
                jnp.where(forward, one, zero),
                jnp.where(forward, one, decay),
                jnp.where(forward, zero, one),
            ],
            axis=0,
        )
    )
    upper = iota((8, 512), 0) < 4
    for i in range(PARTS):
        for copy in copies[i]:
            copy.wait()
        for lane in range(0, PART_W, 512):
            s = slice(lane, lane + 512)
            to = slice(i * PART_W + lane, i * PART_W + lane + 512)
            w = mm(weights, spread_matrix((i * PART_W + lane) // 64, 512))
            for k in range(8):
                r = slice(8 * k, 8 * k + 8)
                even = states_buf[i, 2 * k, :, s]
                odd = states_buf[i, 2 * k + 1, :, s]
                fwd = jnp.where(upper, even, pltpu.roll(odd, 4, 0))
                bwd = jnp.where(upper, pltpu.roll(even, 4, 0), odd)
                extra = part_buf[i, r, s]
                fwd_out[r, to] = w[0:8] * fwd + w[8:16] * extra
                bwd_out[r, to] = w[16:24] * bwd + w[24:32] * extra


def core_states(sending, core, states, part, end, end_other, after):
    states, part = (pltpu.with_memory_space_constraint(x, pltpu.HBM) for x in (states, part))
    dma = pltpu.SemaphoreType.DMA
    return pl.pallas_call(
        functools.partial(core_kernel, sending),
        in_specs=[SCALARS, IN_HBM, IN_HBM, IN_VMEM, IN_VMEM, pl.BlockSpec(memory_space=pl.ANY)],
        out_specs=[IN_VMEM] * 2,
        out_shape=[jax.ShapeDtypeStruct((HALF, W), F32)] * 2,
        scratch_shapes=[
            pltpu.VMEM((PARTS, CHIPS, 8, PART_W), F32), pltpu.VMEM((PARTS, HALF, PART_W), F32),
            dma((PARTS,)), dma((PARTS,)),
        ],
        compiler_params=params(),
        cost_estimate=pl.CostEstimate(flops=2_000_000_000, transcendentals=0, bytes_accessed=8_000_000),
        name="sent_states" if sending else "own_states",
    )(core, states, part, end, end_other, after)


INSIDE_LANES = 512


def inside_kernel(
    v, g, b, c, wide, row, tail, grow, after,
    db_out, dc_out, row_out, col_out, heads_out, v_hi, v_lo, g_hi, g_lo,
    mix, scores, cum3, cum_rows, rate_rows,
):
    step = pl.program_id(0)

    @pl.when(step == 0)
    def _():
        c_hi, c_lo = halves(c[...])
        b_hi, b_lo = halves(b[...])
        scores[...] = mm_nt(c_hi, b_hi) + (mm_nt(c_hi, b_lo) + mm_nt(c_lo, b_hi))
        mix[...] = jnp.zeros_like(mix)
        row_out[...] = jnp.zeros_like(row_out)
        rate, decay, slope, pace = rates(wide, row)
        cum = running_sum(decay)
        for k, part in enumerate(thirds(cum)):
            cum3[:, 128 * k : 128 * k + 128] = part
        cum_rows[...] = cum.T
        rate_rows[...] = rate.T
        heads_out[0] = decay
        heads_out[1] = -pace * slope
        heads_out[2] = jnp.where(rate > 0.0, slope / rate, 0.0)

    causal = iota((128, 128), 0) >= iota((128, 128), 1)
    left = iota((T, 128), 1) < 64
    per_step = INSIDE_LANES // 64
    pick = iota((384, 128), 0) % 128 == step * per_step + iota((384, 128), 1)
    cols = mm(cum3[...], pick.astype(BF16))
    some = pl.ds(pl.multiple_of(step * per_step, per_step), per_step)
    cum_t = cum_rows[some, :]
    rate_t = rate_rows[some, :]
    lane = iota((128, 128), 1)
    sums0 = row_out[0:128, :]
    sums1 = row_out[128:256, :]
    zero = jnp.zeros((), BF16)
    for j in range(per_step):
        head = step * per_step + j
        pair = slice(128 * (j // 2), 128 * (j // 2) + 128)
        v_pair = v[:, pair]
        g_pair = g[:, pair]
        g_head = jnp.where(left if j % 2 == 0 else ~left, g_pair, zero)
        cum_row = cum_t[j : j + 1, :]
        rate_row = rate_t[j : j + 1, :]

        def block(t0, s0):
            t = slice(t0, t0 + 128)
            s = slice(s0, s0 + 128)
            gap = cols[t, j : j + 1] - cum_row[:, s]
            if t0 == s0:
                gap = jnp.where(causal, gap, -1e30)
            part = jnp.exp(gap) * rate_row[:, s] * mm_nt(g_head[t], v_pair[s])
            mix[t, s] += part
            return part * scores[t, s]

        m00 = block(0, 0)
        m10 = block(128, 0)
        m11 = block(128, 128)
        sums0 = jnp.where(lane == head, jnp.sum(m00, axis=1, keepdims=True), sums0)
        sums1 = jnp.where(lane == head, jnp.sum(m10 + m11, axis=1, keepdims=True), sums1)
        col_out[j : j + 1, 0:128] = jnp.sum(m00 + m10, axis=0, keepdims=True)
        col_out[j : j + 1, 128:256] = jnp.sum(m11, axis=0, keepdims=True)
    row_out[0:128, :] = sums0
    row_out[128:256, :] = sums1
    for part in range(0, INSIDE_LANES, LANES):
        s = slice(part, part + LANES)
        spread = spread_matrix(step * per_step + part // 64, LANES)
        v_hi[:, s], v_lo[:, s] = halves(scaled(tail[...], spread, v[:, s]))
        g_hi[:, s], g_lo[:, s] = halves(scaled(grow[...], spread, g[:, s]))

    @pl.when(step == pl.num_programs(0) - 1)
    def _():
        m_hi, m_lo = halves(mix[...])
        b_hi, b_lo = halves(b[...])
        c_hi, c_lo = halves(c[...])
        dc_out[...] = mm(m_hi, b_hi) + (mm(m_hi, b_lo) + mm(m_lo, b_hi))
        db_out[...] = mm_tn(m_hi, c_hi) + (mm_tn(m_hi, c_lo) + mm_tn(m_lo, c_hi))


def inside(v, g, b, c, wide, row, tail, grow, after):
    lanes = pl.BlockSpec((T, INSIDE_LANES), lambda i: (0, i))
    some = pl.BlockSpec((INSIDE_LANES // 64, T), lambda i: (i, 0))
    shape = jax.ShapeDtypeStruct
    outs = (shape((T, N), F32), shape((T, N), F32), shape((T, 128), F32), shape((128, T), F32))
    outs += (shape((3, T, 128), F32),)
    outs += (pltpu.HBM((T, W), BF16),) * 4
    return pl.pallas_call(
        inside_kernel,
        grid=(W // INSIDE_LANES,),
        in_specs=[
            lanes, lanes, whole((T, N)), whole((T, N)), whole((T, 128)), whole((16, 128)),
            whole((T, 256)), whole((T, 256)), pl.BlockSpec(memory_space=pl.ANY),
        ],
        out_specs=[whole((T, N)), whole((T, N)), whole((T, 128)), some, whole((3, T, 128))] + [lanes] * 4,
        out_shape=outs,
        scratch_shapes=[
            pltpu.VMEM((T, T), F32), pltpu.VMEM((T, T), F32), pltpu.VMEM((T, 384), BF16),
            pltpu.VMEM((128, T), F32), pltpu.VMEM((128, T), F32),
        ],
        compiler_params=params("arbitrary"),
        cost_estimate=pl.CostEstimate(flops=20_000_000_000, transcendentals=4_000_000, bytes_accessed=6_000_000),
        name="inside",
    )(v, g, b, c, wide, row, tail, grow, after)


OUTSIDE_LANES = 1024


def outside_kernel(linked, *refs):
    if linked:
        rows_hi, rows_lo, mine, got, other, mine_in, got_in, d_out, sum_out, link_out = refs
    else:
        rows_hi, rows_lo, mine, got, other, d_out, sum_out = refs
    step = pl.program_id(0)

    @pl.when(step == 0)
    def _():
        for ref in (d_out, sum_out) + ((link_out,) if linked else ()):
            ref[...] = jnp.zeros_like(ref)

    gather = gather_matrix(step * (OUTSIDE_LANES // 64), OUTSIDE_LANES)
    state = jnp.concatenate([mine[...], got[...]], axis=0)
    s_hi, s_lo = halves(state)
    both = jnp.concatenate([s_hi, s_lo], axis=0)
    far = mm_nt(rows_hi[...], both)
    d_out[...] += far[:, 0:N] + far[:, N : 2 * N] + mm_nt(rows_lo[...], s_hi)
    o_hi = other[...].astype(BF16)
    o_two = jnp.concatenate([o_hi, o_hi], axis=1)
    total = sum_out[...]
    for lane in range(0, OUTSIDE_LANES, LANES):
        s = slice(lane, lane + LANES)
        term = (rows_hi[:, s].astype(F32) * mm(o_two, both[:, s])).astype(BF16)
        total = total + mm(term, gather[s])
    sum_out[...] = total
    if linked:
        state_in = jnp.concatenate([mine_in[...], got_in[...]], axis=0)
        joint = jnp.broadcast_to(jnp.sum(state_in * state, axis=0, keepdims=True), (8, OUTSIDE_LANES))
        j0, j1, j2 = thirds(joint)
        link_out[...] += mm(j0, gather) + (mm(j1, gather) + mm(j2, gather))


def outside(rows_hi, rows_lo, mine, got, other, *states_in):
    linked = len(states_in) > 0
    lanes = pl.BlockSpec((T, OUTSIDE_LANES), lambda i: (0, i))
    rows = pl.BlockSpec((HALF, OUTSIDE_LANES), lambda i: (0, i))
    shape = jax.ShapeDtypeStruct
    outs = (shape((T, N), F32), shape((T, 128), F32)) + ((shape((8, 128), F32),) if linked else ())
    return pl.pallas_call(
        functools.partial(outside_kernel, linked),
        grid=(W // OUTSIDE_LANES,),
        in_specs=[lanes, lanes, rows, rows, whole((T, N))] + [rows] * len(states_in),
        out_specs=[whole(o.shape) for o in outs],
        out_shape=outs,
        compiler_params=params("arbitrary"),
        cost_estimate=pl.CostEstimate(flops=6_000_000_000, transcendentals=0, bytes_accessed=8_000_000),
        name="outside_back" if linked else "outside_in",
    )(rows_hi, rows_lo, mine, got, other, *states_in)


GRAD_STEPS = 4
GRAD_ROWS = D // GRAD_STEPS
ROWS = D // 32


def grads_kernel(
    core, tok, db_in, dc_in, db_far, dc_far, rows_in, cols_in, x_far, z_far, link, end, heads,
    own, other,
    d_proj, res, head_row,
):
    step = pl.program_id(0)
    which = core[0]

    @pl.when(step == 0)
    def _():
        second = which == 1
        db = db_in[...] + db_far[...]
        dc = dc_in[...] + dc_far[...]
        d_proj[:, 0:N] = jnp.where(second, pltpu.roll(db, HALF, 1), db).astype(BF16)
        d_proj[:, N : 2 * N] = jnp.where(second, pltpu.roll(dc, HALF, 1), dc).astype(BF16)
        z = z_far[...]
        ahead = rows_in[...] + x_far[...]
        behind = jnp.where(iota((T, 128), 1) < HEADS, cols_in[...].T, 0.0) + z
        d0, d1, d2 = thirds(ahead - behind)
        onward = (iota((T, T), 0) <= iota((T, T), 1)).astype(BF16)
        carry = jnp.exp(end[0:1, :]) * link[0:1, :] + jnp.sum(z, axis=0, keepdims=True)
        flux = mm(onward, d0) + (mm(onward, d1) + mm(onward, d2)) + carry
        d_log = jnp.sum(flux * heads[0], axis=0, keepdims=True)
        d_bias = jnp.sum(behind * heads[2] + flux * heads[1], axis=0, keepdims=True)
        head_row[:, 0:128] = jnp.broadcast_to(d_log, (8, 128))
        head_row[:, 128:256] = jnp.broadcast_to(d_bias, (8, 128))

    res[...] = mm_tn(tok[...], d_proj[...])
    for k in range(GRAD_ROWS // (2 * ROWS)):
        own[k, 0:ROWS] = res[pl.ds(2 * ROWS * k + ROWS * which, ROWS), :]
        own[k, ROWS : ROWS + 8] = head_row[...]
        other[k, 0:ROWS] = res[pl.ds(2 * ROWS * k + ROWS * (1 - which), ROWS), :]
        other[k, ROWS : ROWS + 8] = head_row[...]


def grads(core, tok, *parts):
    shape = jax.ShapeDtypeStruct
    pieces = GRAD_ROWS // (2 * ROWS)
    out = pl.BlockSpec((pieces, ROWS + 8, 2 * N), lambda i: (i, 0, 0))
    return pl.pallas_call(
        grads_kernel,
        grid=(GRAD_STEPS,),
        in_specs=[SCALARS, pl.BlockSpec((T, GRAD_ROWS), lambda i: (0, i))] + [whole(p.shape) for p in parts],
        out_specs=[out, out],
        out_shape=[shape((CHIPS, ROWS + 8, 2 * N), F32)] * 2,
        scratch_shapes=[
            pltpu.VMEM((T, 2 * N), BF16), pltpu.VMEM((GRAD_ROWS, 2 * N), F32), pltpu.VMEM((8, 2 * N), F32),
        ],
        compiler_params=params("arbitrary"),
        name="grads",
    )(core, tok, *parts)


def settle_kernel(fire, pieces, last_bc, last_heads, new_bc, new_heads, packed, square, head_square, heads):
    fires = fire[0] > 0
    weight = fire[0].astype(F32)
    total = pieces[0]
    for k in range(1, CHIPS):
        total = total + pieces[k]
    rows = total[0:ROWS]
    heads[...] = jnp.zeros_like(heads)
    heads[0:1, :] = total[ROWS : ROWS + 1, 0:128]
    heads[1:2, :] = total[ROWS : ROWS + 1, 128:256]
    sums = heads[0:2, 0:HEADS]
    last = last_heads[...]
    new_heads[...] = jnp.where(fires, sums, last)
    diff_heads = sums - last
    diff = rows - last_bc[...]
    new_bc[...] = jnp.where(fires, rows, last_bc[...])
    packed[0:ROWS, :] = weight * diff
    packed[ROWS : ROWS + 8, :] = jnp.zeros((8, 2 * N), F32)
    packed[ROWS : ROWS + 2, 0:HEADS] = weight * diff_heads
    lanes = jnp.sum(diff * diff, axis=0, keepdims=True)
    square[...] = jnp.broadcast_to(lanes[:, 0:128] + lanes[:, 128:256], (8, 128))
    head_square[...] = jnp.broadcast_to(jnp.sum(diff_heads * diff_heads, keepdims=True), (8, 128))


def settle(fire, pieces, last_bc, last_heads):
    shape = jax.ShapeDtypeStruct
    vmem = pl.BlockSpec(memory_space=pltpu.VMEM)
    return pl.pallas_call(
        settle_kernel,
        in_specs=[SCALARS, vmem, vmem, vmem],
        out_specs=[vmem] * 5,
        out_shape=[
            shape((ROWS, 2 * N), F32), shape((2, HEADS), F32), shape((ROWS + 8, 2 * N), F32),
            shape((8, 128), F32), shape((8, 128), F32),
        ],
        scratch_shapes=[pltpu.VMEM((8, 128), F32)],
        compiler_params=params(),
        name="settle",
    )(fire, pieces, last_bc, last_heads)


def ring_sum(x0, x1, x2, x3):
    return (x0 + x2) + (x1 + x3)


def finish_kernel(
    p0, p1, p2, p3, s0, s1, s2, s3, head_square, total_bc, total_heads, new_bc, new_heads, trigger
):
    fired = ring_sum(p0[...], p1[...], p2[...], p3[...])
    new_bc[...] = total_bc[...] + fired[0:ROWS]
    new_heads[...] = total_heads[...] + fired[ROWS : ROWS + 2, 0:HEADS]
    square = jnp.sum(ring_sum(s0[...], s1[...], s2[...], s3[...])[0:1], keepdims=True)
    trigger[...] = jnp.sqrt(square + head_square[0:1, 0:1] + 1e-06)


def finish(parts, squares, head_square, total_bc, total_heads):
    shape = jax.ShapeDtypeStruct
    vmem = pl.BlockSpec(memory_space=pltpu.VMEM)
    return pl.pallas_call(
        finish_kernel,
        in_specs=[vmem] * 11,
        out_specs=[vmem] * 3,
        out_shape=[shape((ROWS, 2 * N), F32), shape((2, HEADS), F32), shape((1, 1), F32)],
        compiler_params=params(),
        name="finish",
    )(*parts, *squares, head_square, total_bc, total_heads)


def on_ring(x, axis):
    return [x] + [lax.ppermute(x, axis, [(r, (r + k) % 4) for r in range(4)]) for k in (1, 2, 3)]


def all_to_all(x, axis):
    return lax.all_to_all(x, axis, 0, 0, tiled=True)


def local(
    tokens, values, out_grad, w_bc, w_dt, a_log, dt_bias, fire_flags, last_bc, last_heads, total_bc, total_heads
):
    tok, v, g = tokens[0], values[0], out_grad[0]
    core = lax.axis_index("c").astype(jnp.int32).reshape(1)
    own, other, b, c, tail, grow, wide, row, end = front(
        core, tok, w_bc, w_dt.T, a_log.reshape(1, HEADS), dt_bias.reshape(1, HEADS), v, g
    )
    end_other = lax.ppermute(end, "c", CORE_SWAP)
    arrived = lax.ppermute(other, "c", CORE_SWAP)
    terms = chip_terms(core, own, arrived, end, end_other)
    before = scan_chips(all_to_all(terms, RING))
    states = all_to_all(before, RING)
    db_in, dc_in, rows_in, cols_in, heads, v_hi, v_lo, g_hi, g_lo = inside(
        v, g, b, c, wide, row, tail, grow, before
    )
    sent_in, sent_back = core_states(True, core, states, own, end, end_other, rows_in)
    got_in = lax.ppermute(sent_in, "c", CORE_SWAP)
    got_back = lax.ppermute(sent_back, "c", CORE_SWAP)
    mine_in, mine_back = core_states(False, core, states, arrived, end, end_other, rows_in)
    dc_far, x_far = outside(g_hi, g_lo, mine_in, got_in, c)
    db_far, z_far, link = outside(v_hi, v_lo, mine_back, got_back, b, mine_in, got_in)
    rows_own, rows_other = grads(
        core, tok, db_in, dc_in, db_far, dc_far, rows_in, cols_in, x_far, z_far, link, end, heads
    )
    rows = rows_own + lax.ppermute(rows_other, "c", CORE_SWAP)
    new_bc, new_heads, packed, square, head_square = settle(
        fire_flags, all_to_all(rows, RING), last_bc[0], last_heads[0]
    )
    on_chip = square + lax.ppermute(square, "c", CORE_SWAP)
    squares = on_ring(ring_sum(*on_ring(on_chip, "y")), "z")
    total_bc, total_heads, trigger = finish(on_ring(packed, "dp"), squares, head_square, total_bc, total_heads)
    return total_bc, total_heads, new_bc[None], new_heads[None], trigger.reshape(1)


def solution(mesh):
    split = Mesh(mesh.devices.reshape(mesh.shape["dp"], 4, 4, 2), ("dp",) + SEQ)
    rows = P("dp", SEQ, None)
    in_specs = (
        rows, rows, rows, P(), P(), P(), P(), P("dp"), rows, P("dp", None, None), P(SEQ, None), P(),
    )
    out_specs = (P(SEQ, None), P(), rows, P("dp", None, None), P("dp"))
    return jax.shard_map(local, mesh=split, in_specs=in_specs, out_specs=out_specs, check_vma=False)
```

```python
import functools

import jax
import jax.numpy as jnp
from jax import lax
from jax.experimental import pallas as pl
from jax.experimental.pallas import tpu as pltpu
from jax.sharding import Mesh
from jax.sharding import PartitionSpec as P

F32 = jnp.float32
BF16 = jnp.bfloat16
T = 256
D = 2560
N = 128
HEADS = 80
W = 5120
HALF = 64
CHIPS = 16
SEQ = ("z", "y", "c")
RING = ("z", "y")
CORE_SWAP = [(0, 1), (1, 0)]


def iota(shape, dim):
    return lax.broadcasted_iota(jnp.int32, shape, dim)


def halves(x):
    high = x.astype(BF16)
    return high, (x - high.astype(F32)).astype(BF16)


def thirds(x):
    high = x.astype(BF16)
    rest = x - high.astype(F32)
    mid = rest.astype(BF16)
    return high, mid, (rest - mid.astype(F32)).astype(BF16)


def mm(a, b):
    return jnp.dot(a, b, preferred_element_type=F32)


def mm_nt(a, b):
    return lax.dot_general(a, b, (((1,), (1,)), ((), ())), preferred_element_type=F32)


def mm_tn(a, b):
    return lax.dot_general(a, b, (((0,), (0,)), ((), ())), preferred_element_type=F32)


def spread_matrix(first_head, lanes):
    head = iota((256, lanes), 0) % 128
    return (head == first_head + iota((256, lanes), 1) // 64).astype(BF16)


def gather_matrix(first_head, lanes):
    return (first_head + iota((lanes, 128), 0) // 64 == iota((lanes, 128), 1)).astype(BF16)


def paired(x):
    return jnp.concatenate(halves(x), axis=1)


def whole(shape):
    return pl.BlockSpec(shape, lambda *_: (0,) * len(shape))


SCALARS = pl.BlockSpec(memory_space=pltpu.SMEM)


def params(*semantics):
    return pltpu.CompilerParams(dimension_semantics=semantics, vmem_limit_bytes=20 << 20)


LANES = 256
STEPS = W // LANES


def scaled(pair, spread, rows):
    return mm(pair, spread) * rows.astype(F32)


def three(left, right):
    hi, lo = halves(right)
    wide = mm(left[...], hi)
    return wide[0:N] + (wide[N : 2 * N] + mm(left[0:N], lo))


PARTS = 5
PART_D = D // PARTS
PART_W = W // PARTS
IN_HBM = pl.BlockSpec(memory_space=pltpu.HBM)
IN_VMEM = pl.BlockSpec(memory_space=pltpu.VMEM)


def cut(i, width):
    return slice(i * width, (i + 1) * width)


def rates(wide, row):
    x = wide[...] + row[8:9, :]
    small = jnp.exp(-jnp.abs(x))
    rate = jnp.maximum(x, 0.0) + jnp.log1p(small)
    slope = jnp.where(x >= 0.0, 1.0, small) / (1.0 + small)
    pace = jnp.exp(row[0:1, :])
    return rate, -rate * pace, slope, pace


def running_sum(decay):
    upto = (iota((T, T), 0) >= iota((T, T), 1)).astype(BF16)
    d0, d1, d2 = thirds(decay)
    return mm(upto, d2) + mm(upto, d1) + mm(upto, d0)


def front_kernel(
    core, tok, w_bc, w_dt, a_log, dt_bias, v, g,
    own, other, b_out, c_out, tail_out, grow_out, wide, row, end_out,
    tok_buf, bc_buf, dt_buf, log_buf, bias_buf, v_buf, g_buf, bt, ct, hi_buf, lo_buf,
    tok_sem, bc_sem, dt_sem, row_sem, v_sem, g_sem,
):
    copies = []
    for i in range(PARTS):
        k = cut(i, PART_D)
        copies.append((
            pltpu.make_async_copy(tok.at[:, k], tok_buf.at[i], tok_sem.at[i]),
            pltpu.make_async_copy(w_bc.at[k, :], bc_buf.at[i], bc_sem.at[i]),
            pltpu.make_async_copy(w_dt.at[:, k], dt_buf.at[i], dt_sem.at[i]),
        ))
    small = (
        pltpu.make_async_copy(a_log, log_buf, row_sem.at[0]),
        pltpu.make_async_copy(dt_bias, bias_buf, row_sem.at[1]),
    )
    rows_in = [
        (
            pltpu.make_async_copy(v.at[:, cut(i, PART_W)], v_buf.at[i], v_sem.at[i]),
            pltpu.make_async_copy(g.at[:, cut(i, PART_W)], g_buf.at[i], g_sem.at[i]),
        )
        for i in range(PARTS)
    ]
    for group in copies:
        for copy in group:
            copy.start()
    for copy in small:
        copy.start()
    for group in rows_in:
        for copy in group:
            copy.start()
    row[...] = jnp.zeros_like(row)
    wide[...] = jnp.zeros_like(wide)
    projected = None
    raw_dt = None
    for i in range(PARTS):
        for copy in copies[i]:
            copy.wait()
        u = tok_buf[i]
        part = mm(u, bc_buf[i])
        part_dt = mm_nt(u, dt_buf[i])
        projected = part if i == 0 else projected + part
        raw_dt = part_dt if i == 0 else raw_dt + part_dt
    for copy in small:
        copy.wait()
    row[0:1, 0:HEADS] = log_buf[...]
    row[8:9, 0:HEADS] = bias_buf[...]
    wide[:, 0:HEADS] = raw_dt
    second = core[0] == 1
    b = projected[:, 0:N]
    c = projected[:, N : 2 * N]
    b = jnp.where(second, pltpu.roll(b, HALF, 1), b)
    c = jnp.where(second, pltpu.roll(c, HALF, 1), c)
    b_out[...] = b
    c_out[...] = c
    bt_hi, bt_lo = halves(b.T)
    ct_hi, ct_lo = halves(c.T)
    bt[0:N, :] = bt_hi
    bt[N : 2 * N, :] = bt_lo
    ct[0:N, :] = ct_hi
    ct[N : 2 * N, :] = ct_lo
    rate, decay = rates(wide, row)[0:2]
    cum = running_sum(decay)
    end = cum[T - 1 : T, :]
    tail_out[...] = paired(jnp.exp(end - cum) * rate)
    grow_out[...] = paired(jnp.exp(cum))
    end_out[...] = jnp.broadcast_to(end, (8, 128))

    def add_part(i, _):
        start = pl.multiple_of(i * PART_W, PART_W)
        lanes = pl.ds(start, PART_W)
        pltpu.make_async_copy(v.at[:, lanes], v_buf.at[i], v_sem.at[i]).wait()
        pltpu.make_async_copy(g.at[:, lanes], g_buf.at[i], g_sem.at[i]).wait()
        for lane in range(0, PART_W, LANES):
            s = slice(lane, lane + LANES)
            spread = spread_matrix(i * (PART_W // 64) + lane // 64, LANES)
            for n, (pair, rows) in enumerate(((tail_out, v_buf), (grow_out, g_buf))):
                hi, lo = halves(scaled(pair[...], spread, rows[i, :, s]))
                hi_buf[n, :, s] = hi
                lo_buf[n, :, s] = lo
        for lane in range(0, PART_W, 2 * LANES):
            s = slice(lane, lane + 2 * LANES)
            to = pl.ds(start + lane, 2 * LANES)
            for n, left in enumerate((bt, ct)):
                hi = hi_buf[n, :, s]
                wide_sum = mm(left[...], hi)
                total = wide_sum[0:N] + (wide_sum[N : 2 * N] + mm(left[0:N], lo_buf[n, :, s]))
                r = slice(HALF * n, HALF * n + HALF)
                own[r, to] = total[0:HALF]
                other[r, to] = total[HALF:N]
        return 0

    lax.fori_loop(0, PARTS, add_part, 0)


def front(core, tok, w_bc, w_dt, a_log, dt_bias, v, g):
    shape = jax.ShapeDtypeStruct
    vmem = pltpu.VMEM
    dma = pltpu.SemaphoreType.DMA
    outs = (
        shape((N, W), F32), shape((N, W), F32), shape((T, N), F32), shape((T, N), F32),
        shape((T, 256), BF16), shape((T, 256), BF16), shape((T, 128), F32), shape((16, 128), F32), shape((8, 128), F32),
    )
    tok, w_bc, w_dt, a_log, dt_bias, v, g = (
        pltpu.with_memory_space_constraint(x, pltpu.HBM) for x in (tok, w_bc, w_dt, a_log, dt_bias, v, g)
    )
    return pl.pallas_call(
        front_kernel,
        in_specs=[SCALARS] + [IN_HBM] * 7,
        out_specs=[IN_VMEM] * len(outs),
        out_shape=outs,
        scratch_shapes=[
            vmem((PARTS, T, PART_D), BF16), vmem((PARTS, PART_D, 2 * N), BF16), vmem((PARTS, HEADS, PART_D), BF16),
            vmem((1, HEADS), F32), vmem((1, HEADS), F32),
            vmem((PARTS, T, PART_W), BF16), vmem((PARTS, T, PART_W), BF16),
            vmem((2 * N, T), BF16), vmem((2 * N, T), BF16), vmem((2, T, PART_W), BF16), vmem((2, T, PART_W), BF16),
            dma((PARTS,)), dma((PARTS,)), dma((PARTS,)), dma((2,)), dma((PARTS,)), dma((PARTS,)),
        ],
        compiler_params=pltpu.CompilerParams(vmem_limit_bytes=28 << 20),
        name="front",
    )(core, tok, w_bc, w_dt, a_log, dt_bias, v, g)


def chip_kernel(core, own, arrived, end, end_other, out):
    second = core[0] == 1
    mine = jnp.exp(end[...])
    theirs = jnp.exp(end_other[...])
    one = jnp.ones_like(mine)
    weights = jnp.concatenate(
        [
            jnp.where(second, one, theirs),
            jnp.where(second, mine, one),
            jnp.where(second, theirs, one),
            jnp.where(second, one, mine),
        ],
        axis=0,
    )
    weights = paired(weights)
    upper = iota((8, 512), 0) < 4
    for lane in range(0, W, 512):
        s = slice(lane, lane + 512)
        scale = mm(weights, spread_matrix(lane // 64, 512))
        for k in range(8):
            r = slice(8 * k, 8 * k + 8)
            q = slice(HALF + 8 * k, HALF + 8 * k + 8)
            fwd = scale[0:8] * own[r, s] + scale[8:16] * arrived[r, s]
            bwd = scale[16:24] * own[q, s] + scale[24:32] * arrived[q, s]
            out[2 * k, :, s] = jnp.where(upper, fwd, pltpu.roll(bwd, 4, 0))
            out[2 * k + 1, :, s] = jnp.where(upper, pltpu.roll(fwd, 4, 0), bwd)
    total = end[...] + end_other[...]
    for k in range(CHIPS):
        out[k, :, W : W + 128] = total


def chip_terms(core, own, arrived, end, end_other):
    return pl.pallas_call(
        chip_kernel,
        in_specs=[SCALARS] + [pl.BlockSpec(memory_space=pltpu.VMEM)] * 4,
        out_specs=pl.BlockSpec(memory_space=pltpu.VMEM),
        out_shape=jax.ShapeDtypeStruct((CHIPS, 8, W + 128), F32),
        compiler_params=params(),
        name="chip_terms",
    )(core, own, arrived, end, end_other)


def scan_kernel(terms, out, out_buf, out_sem):
    decays = paired(jnp.exp(terms[:, :, W : W + 128].reshape(CHIPS * 8, 128)))
    upper = iota((8, 512), 0) < 4
    copies = []
    for lane in range(0, W, 512):
        s = slice(lane, lane + 512)
        decay = mm(decays, spread_matrix(lane // 64, 512))
        state = jnp.zeros((8, 512), F32)
        for k in range(CHIPS):
            m = CHIPS - 1 - k
            out_buf[k, 0:4, s] = state[0:4]
            out_buf[m, 4:8, s] = state[4:8]
            here = jnp.where(upper, terms[k, :, s], terms[m, :, s])
            rate = jnp.where(upper, decay[8 * k : 8 * k + 8], decay[8 * m : 8 * m + 8])
            state = rate * state + here
        copy = pltpu.make_async_copy(out_buf.at[:, :, s], out.at[:, :, s], out_sem.at[lane // 512])
        copy.start()
        copies.append(copy)
    for copy in copies:
        copy.wait()


def scan_chips(terms):
    return pl.pallas_call(
        scan_kernel,
        in_specs=[IN_VMEM],
        out_specs=IN_HBM,
        out_shape=pltpu.HBM((CHIPS, 8, W), F32),
        scratch_shapes=[pltpu.VMEM((CHIPS, 8, W), F32), pltpu.SemaphoreType.DMA((W // 512,))],
        compiler_params=params(),
        name="scan_chips",
    )(terms)


def core_kernel(
    sending, core, states, part, end, end_other, after, fwd_out, bwd_out, states_buf, part_buf, states_sem, part_sem
):
    lanes = [cut(i, PART_W) for i in range(PARTS)]
    row = pl.multiple_of(HALF * (core[0] if sending else 1 - core[0]), HALF)
    copies = [
        (
            pltpu.make_async_copy(states.at[:, :, s], states_buf.at[i], states_sem.at[i]),
            pltpu.make_async_copy(part.at[pl.ds(row, HALF), s], part_buf.at[i], part_sem.at[i]),
        )
        for i, s in enumerate(lanes)
    ]
    for group in copies:
        for copy in group:
            copy.start()
    forward = (core[0] == 0) == sending
    decay = jnp.exp(jnp.where(sending, end[...], end_other[...]))
    one = jnp.ones_like(decay)
    zero = jnp.zeros_like(decay)
    weights = paired(
        jnp.concatenate(
            [
                jnp.where(forward, decay, one),
                jnp.where(forward, one, zero),
                jnp.where(forward, one, decay),
                jnp.where(forward, zero, one),
            ],
            axis=0,
        )
    )
    upper = iota((8, 512), 0) < 4
    for i in range(PARTS):
        for copy in copies[i]:
            copy.wait()
        for lane in range(0, PART_W, 512):
            s = slice(lane, lane + 512)
            to = slice(i * PART_W + lane, i * PART_W + lane + 512)
            w = mm(weights, spread_matrix((i * PART_W + lane) // 64, 512))
            for k in range(8):
                r = slice(8 * k, 8 * k + 8)
                even = states_buf[i, 2 * k, :, s]
                odd = states_buf[i, 2 * k + 1, :, s]
                fwd = jnp.where(upper, even, pltpu.roll(odd, 4, 0))
                bwd = jnp.where(upper, pltpu.roll(even, 4, 0), odd)
                extra = part_buf[i, r, s]
                fwd_out[r, to] = w[0:8] * fwd + w[8:16] * extra
                bwd_out[r, to] = w[16:24] * bwd + w[24:32] * extra


def core_states(sending, core, states, part, end, end_other, after):
    states, part = (pltpu.with_memory_space_constraint(x, pltpu.HBM) for x in (states, part))
    dma = pltpu.SemaphoreType.DMA
    return pl.pallas_call(
        functools.partial(core_kernel, sending),
        in_specs=[SCALARS, IN_HBM, IN_HBM, IN_VMEM, IN_VMEM, pl.BlockSpec(memory_space=pl.ANY)],
        out_specs=[IN_VMEM] * 2,
        out_shape=[jax.ShapeDtypeStruct((HALF, W), F32)] * 2,
        scratch_shapes=[
            pltpu.VMEM((PARTS, CHIPS, 8, PART_W), F32), pltpu.VMEM((PARTS, HALF, PART_W), F32),
            dma((PARTS,)), dma((PARTS,)),
        ],
        compiler_params=params(),
        cost_estimate=pl.CostEstimate(flops=2_000_000_000, transcendentals=0, bytes_accessed=8_000_000),
        name="sent_states" if sending else "own_states",
    )(core, states, part, end, end_other, after)


INSIDE_LANES = 512


def inside_kernel(
    v, g, b, c, wide, row, tail, grow, after,
    db_out, dc_out, row_out, col_out, heads_out, v_hi, v_lo, g_hi, g_lo,
    mix, scores, cum3, cum_rows, rate_rows,
):
    step = pl.program_id(0)

    @pl.when(step == 0)
    def _():
        c_hi, c_lo = halves(c[...])
        b_hi, b_lo = halves(b[...])
        scores[...] = mm_nt(c_hi, b_hi) + (mm_nt(c_hi, b_lo) + mm_nt(c_lo, b_hi))
        mix[...] = jnp.zeros_like(mix)
        row_out[...] = jnp.zeros_like(row_out)
        rate, decay, slope, pace = rates(wide, row)
        cum = running_sum(decay)
        for k, part in enumerate(thirds(cum)):
            cum3[:, 128 * k : 128 * k + 128] = part
        cum_rows[...] = cum.T
        rate_rows[...] = rate.T
        heads_out[0] = decay
        heads_out[1] = -pace * slope
        heads_out[2] = jnp.where(rate > 0.0, slope / rate, 0.0)

    causal = iota((128, 128), 0) >= iota((128, 128), 1)
    left = iota((T, 128), 1) < 64
    per_step = INSIDE_LANES // 64
    pick = iota((384, 128), 0) % 128 == step * per_step + iota((384, 128), 1)
    cols = mm(cum3[...], pick.astype(BF16))
    some = pl.ds(pl.multiple_of(step * per_step, per_step), per_step)
    cum_t = cum_rows[some, :]
    rate_t = rate_rows[some, :]
    lane = iota((128, 128), 1)
    sums0 = row_out[0:128, :]
    sums1 = row_out[128:256, :]
    zero = jnp.zeros((), BF16)
    for j in range(per_step):
        head = step * per_step + j
        pair = slice(128 * (j // 2), 128 * (j // 2) + 128)
        v_pair = v[:, pair]
        g_pair = g[:, pair]
        g_head = jnp.where(left if j % 2 == 0 else ~left, g_pair, zero)
        cum_row = cum_t[j : j + 1, :]
        rate_row = rate_t[j : j + 1, :]

        def block(t0, s0):
            t = slice(t0, t0 + 128)
            s = slice(s0, s0 + 128)
            gap = cols[t, j : j + 1] - cum_row[:, s]
            if t0 == s0:
                gap = jnp.where(causal, gap, -1e30)
            part = jnp.exp(gap) * rate_row[:, s] * mm_nt(g_head[t], v_pair[s])
            mix[t, s] += part
            return part * scores[t, s]

        m00 = block(0, 0)
        m10 = block(128, 0)
        m11 = block(128, 128)
        sums0 = jnp.where(lane == head, jnp.sum(m00, axis=1, keepdims=True), sums0)
        sums1 = jnp.where(lane == head, jnp.sum(m10 + m11, axis=1, keepdims=True), sums1)
        col_out[j : j + 1, 0:128] = jnp.sum(m00 + m10, axis=0, keepdims=True)
        col_out[j : j + 1, 128:256] = jnp.sum(m11, axis=0, keepdims=True)
    row_out[0:128, :] = sums0
    row_out[128:256, :] = sums1
    for part in range(0, INSIDE_LANES, LANES):
        s = slice(part, part + LANES)
        spread = spread_matrix(step * per_step + part // 64, LANES)
        v_hi[:, s], v_lo[:, s] = halves(scaled(tail[...], spread, v[:, s]))
        g_hi[:, s], g_lo[:, s] = halves(scaled(grow[...], spread, g[:, s]))

    @pl.when(step == pl.num_programs(0) - 1)
    def _():
        m_hi, m_lo = halves(mix[...])
        b_hi, b_lo = halves(b[...])
        c_hi, c_lo = halves(c[...])
        dc_out[...] = mm(m_hi, b_hi) + (mm(m_hi, b_lo) + mm(m_lo, b_hi))
        db_out[...] = mm_tn(m_hi, c_hi) + (mm_tn(m_hi, c_lo) + mm_tn(m_lo, c_hi))


def inside(v, g, b, c, wide, row, tail, grow, after):
    after = pltpu.with_memory_space_constraint(after, pltpu.HBM)
    lanes = pl.BlockSpec((T, INSIDE_LANES), lambda i: (0, i))
    some = pl.BlockSpec((INSIDE_LANES // 64, T), lambda i: (i, 0))
    shape = jax.ShapeDtypeStruct
    outs = (shape((T, N), F32), shape((T, N), F32), shape((T, 128), F32), shape((128, T), F32))
    outs += (shape((3, T, 128), F32),)
    outs += (pltpu.HBM((T, W), BF16),) * 4
    return pl.pallas_call(
        inside_kernel,
        grid=(W // INSIDE_LANES,),
        in_specs=[
            lanes, lanes, whole((T, N)), whole((T, N)), whole((T, 128)), whole((16, 128)),
            whole((T, 256)), whole((T, 256)), pl.BlockSpec(memory_space=pl.ANY),
        ],
        out_specs=[whole((T, N)), whole((T, N)), whole((T, 128)), some, whole((3, T, 128))] + [lanes] * 4,
        out_shape=outs,
        scratch_shapes=[
            pltpu.VMEM((T, T), F32), pltpu.VMEM((T, T), F32), pltpu.VMEM((T, 384), BF16),
            pltpu.VMEM((128, T), F32), pltpu.VMEM((128, T), F32),
        ],
        compiler_params=params("arbitrary"),
        cost_estimate=pl.CostEstimate(flops=20_000_000_000, transcendentals=4_000_000, bytes_accessed=6_000_000),
        name="inside",
    )(v, g, b, c, wide, row, tail, grow, after)


OUTSIDE_LANES = 2560


def outside_kernel(linked, *refs):
    if linked:
        rows_hi, rows_lo, mine, got, other, mine_in, got_in, d_out, sum_out, link_out = refs
    else:
        rows_hi, rows_lo, mine, got, other, d_out, sum_out = refs
    step = pl.program_id(0)

    @pl.when(step == 0)
    def _():
        for ref in (d_out, sum_out) + ((link_out,) if linked else ()):
            ref[...] = jnp.zeros_like(ref)

    gather = gather_matrix(step * (OUTSIDE_LANES // 64), OUTSIDE_LANES)
    state = jnp.concatenate([mine[...], got[...]], axis=0)
    s_hi, s_lo = halves(state)
    both = jnp.concatenate([s_hi, s_lo], axis=0)
    far = mm_nt(rows_hi[...], both)
    d_out[...] += far[:, 0:N] + far[:, N : 2 * N] + mm_nt(rows_lo[...], s_hi)
    o_hi = other[...].astype(BF16)
    o_two = jnp.concatenate([o_hi, o_hi], axis=1)
    total = sum_out[...]
    for lane in range(0, OUTSIDE_LANES, LANES):
        s = slice(lane, lane + LANES)
        term = (rows_hi[:, s].astype(F32) * mm(o_two, both[:, s])).astype(BF16)
        total = total + mm(term, gather[s])
    sum_out[...] = total
    if linked:
        state_in = jnp.concatenate([mine_in[...], got_in[...]], axis=0)
        joint = jnp.broadcast_to(jnp.sum(state_in * state, axis=0, keepdims=True), (8, OUTSIDE_LANES))
        j0, j1, j2 = thirds(joint)
        link_out[...] += mm(j0, gather) + (mm(j1, gather) + mm(j2, gather))


def outside(rows_hi, rows_lo, mine, got, other, *states_in):
    linked = len(states_in) > 0
    lanes = pl.BlockSpec((T, OUTSIDE_LANES), lambda i: (0, i))
    rows = pl.BlockSpec((HALF, OUTSIDE_LANES), lambda i: (0, i))
    shape = jax.ShapeDtypeStruct
    outs = (shape((T, N), F32), shape((T, 128), F32)) + ((shape((8, 128), F32),) if linked else ())
    return pl.pallas_call(
        functools.partial(outside_kernel, linked),
        grid=(W // OUTSIDE_LANES,),
        in_specs=[lanes, lanes, rows, rows, whole((T, N))] + [rows] * len(states_in),
        out_specs=[whole(o.shape) for o in outs],
        out_shape=outs,
        compiler_params=params("arbitrary"),
        cost_estimate=pl.CostEstimate(flops=6_000_000_000, transcendentals=0, bytes_accessed=8_000_000),
        name="outside_back" if linked else "outside_in",
    )(rows_hi, rows_lo, mine, got, other, *states_in)


GRAD_STEPS = 4
GRAD_ROWS = D // GRAD_STEPS
ROWS = D // 32


def grads_kernel(
    core, tok, db_in, dc_in, db_far, dc_far, rows_in, cols_in, x_far, z_far, link, end, heads,
    own, other,
    d_proj, res, head_row,
):
    step = pl.program_id(0)
    which = core[0]

    @pl.when(step == 0)
    def _():
        second = which == 1
        db = db_in[...] + db_far[...]
        dc = dc_in[...] + dc_far[...]
        d_proj[:, 0:N] = jnp.where(second, pltpu.roll(db, HALF, 1), db).astype(BF16)
        d_proj[:, N : 2 * N] = jnp.where(second, pltpu.roll(dc, HALF, 1), dc).astype(BF16)
        z = z_far[...]
        ahead = rows_in[...] + x_far[...]
        behind = jnp.where(iota((T, 128), 1) < HEADS, cols_in[...].T, 0.0) + z
        d0, d1, d2 = thirds(ahead - behind)
        onward = (iota((T, T), 0) <= iota((T, T), 1)).astype(BF16)
        carry = jnp.exp(end[0:1, :]) * link[0:1, :] + jnp.sum(z, axis=0, keepdims=True)
        flux = mm(onward, d0) + (mm(onward, d1) + mm(onward, d2)) + carry
        d_log = jnp.sum(flux * heads[0], axis=0, keepdims=True)
        d_bias = jnp.sum(behind * heads[2] + flux * heads[1], axis=0, keepdims=True)
        head_row[:, 0:128] = jnp.broadcast_to(d_log, (8, 128))
        head_row[:, 128:256] = jnp.broadcast_to(d_bias, (8, 128))

    res[...] = mm_tn(tok[...], d_proj[...])
    for k in range(GRAD_ROWS // (2 * ROWS)):
        own[k, 0:ROWS] = res[pl.ds(2 * ROWS * k + ROWS * which, ROWS), :]
        own[k, ROWS : ROWS + 8] = head_row[...]
        other[k, 0:ROWS] = res[pl.ds(2 * ROWS * k + ROWS * (1 - which), ROWS), :]
        other[k, ROWS : ROWS + 8] = head_row[...]


def grads(core, tok, *parts):
    shape = jax.ShapeDtypeStruct
    pieces = GRAD_ROWS // (2 * ROWS)
    out = pl.BlockSpec((pieces, ROWS + 8, 2 * N), lambda i: (i, 0, 0))
    return pl.pallas_call(
        grads_kernel,
        grid=(GRAD_STEPS,),
        in_specs=[SCALARS, pl.BlockSpec((T, GRAD_ROWS), lambda i: (0, i))] + [whole(p.shape) for p in parts],
        out_specs=[out, out],
        out_shape=[shape((CHIPS, ROWS + 8, 2 * N), F32)] * 2,
        scratch_shapes=[
            pltpu.VMEM((T, 2 * N), BF16), pltpu.VMEM((GRAD_ROWS, 2 * N), F32), pltpu.VMEM((8, 2 * N), F32),
        ],
        compiler_params=params("arbitrary"),
        name="grads",
    )(core, tok, *parts)


def settle_kernel(fire, pieces, last_bc, last_heads, new_bc, new_heads, packed, square, head_square, heads):
    fires = fire[0] > 0
    weight = fire[0].astype(F32)
    total = pieces[0]
    for k in range(1, CHIPS):
        total = total + pieces[k]
    rows = total[0:ROWS]
    heads[...] = jnp.zeros_like(heads)
    heads[0:1, :] = total[ROWS : ROWS + 1, 0:128]
    heads[1:2, :] = total[ROWS : ROWS + 1, 128:256]
    sums = heads[0:2, 0:HEADS]
    last = last_heads[...]
    new_heads[...] = jnp.where(fires, sums, last)
    diff_heads = sums - last
    diff = rows - last_bc[...]
    new_bc[...] = jnp.where(fires, rows, last_bc[...])
    packed[0:ROWS, :] = weight * diff
    packed[ROWS : ROWS + 8, :] = jnp.zeros((8, 2 * N), F32)
    packed[ROWS : ROWS + 2, 0:HEADS] = weight * diff_heads
    lanes = jnp.sum(diff * diff, axis=0, keepdims=True)
    square[...] = jnp.broadcast_to(lanes[:, 0:128] + lanes[:, 128:256], (8, 128))
    head_square[...] = jnp.broadcast_to(jnp.sum(diff_heads * diff_heads, keepdims=True), (8, 128))


def settle(fire, pieces, last_bc, last_heads):
    shape = jax.ShapeDtypeStruct
    vmem = pl.BlockSpec(memory_space=pltpu.VMEM)
    return pl.pallas_call(
        settle_kernel,
        in_specs=[SCALARS, vmem, vmem, vmem],
        out_specs=[vmem] * 5,
        out_shape=[
            shape((ROWS, 2 * N), F32), shape((2, HEADS), F32), shape((ROWS + 8, 2 * N), F32),
            shape((8, 128), F32), shape((8, 128), F32),
        ],
        scratch_shapes=[pltpu.VMEM((8, 128), F32)],
        compiler_params=params(),
        name="settle",
    )(fire, pieces, last_bc, last_heads)


def ring_sum(x0, x1, x2, x3):
    return (x0 + x2) + (x1 + x3)


def finish_kernel(
    p0, p1, p2, p3, s0, s1, s2, s3, head_square, total_bc, total_heads, new_bc, new_heads, trigger
):
    fired = ring_sum(p0[...], p1[...], p2[...], p3[...])
    new_bc[...] = total_bc[...] + fired[0:ROWS]
    new_heads[...] = total_heads[...] + fired[ROWS : ROWS + 2, 0:HEADS]
    square = jnp.sum(ring_sum(s0[...], s1[...], s2[...], s3[...])[0:1], keepdims=True)
    trigger[...] = jnp.sqrt(square + head_square[0:1, 0:1] + 1e-06)


def finish(parts, squares, head_square, total_bc, total_heads):
    shape = jax.ShapeDtypeStruct
    vmem = pl.BlockSpec(memory_space=pltpu.VMEM)
    return pl.pallas_call(
        finish_kernel,
        in_specs=[vmem] * 11,
        out_specs=[vmem] * 3,
        out_shape=[shape((ROWS, 2 * N), F32), shape((2, HEADS), F32), shape((1, 1), F32)],
        compiler_params=params(),
        name="finish",
    )(*parts, *squares, head_square, total_bc, total_heads)


def on_ring(x, axis):
    return [x] + [lax.ppermute(x, axis, [(r, (r + k) % 4) for r in range(4)]) for k in (1, 2, 3)]


def all_to_all(x, axis):
    return lax.all_to_all(x, axis, 0, 0, tiled=True)


def local(
    tokens, values, out_grad, w_bc, w_dt, a_log, dt_bias, fire_flags, last_bc, last_heads, total_bc, total_heads
):
    tok, v, g = tokens[0], values[0], out_grad[0]
    core = lax.axis_index("c").astype(jnp.int32).reshape(1)
    own, other, b, c, tail, grow, wide, row, end = front(
        core, tok, w_bc, w_dt.T, a_log.reshape(1, HEADS), dt_bias.reshape(1, HEADS), v, g
    )
    end_other = lax.ppermute(end, "c", CORE_SWAP)
    arrived = lax.ppermute(other, "c", CORE_SWAP)
    terms = chip_terms(core, own, arrived, end, end_other)
    before = scan_chips(all_to_all(terms, RING))
    states = all_to_all(before, RING)
    db_in, dc_in, rows_in, cols_in, heads, v_hi, v_lo, g_hi, g_lo = inside(
        v, g, b, c, wide, row, tail, grow, before
    )
    sent_in, sent_back = core_states(True, core, states, own, end, end_other, rows_in)
    got_in = lax.ppermute(sent_in, "c", CORE_SWAP)
    got_back = lax.ppermute(sent_back, "c", CORE_SWAP)
    mine_in, mine_back = core_states(False, core, states, arrived, end, end_other, rows_in)
    dc_far, x_far = outside(g_hi, g_lo, mine_in, got_in, c)
    db_far, z_far, link = outside(v_hi, v_lo, mine_back, got_back, b, mine_in, got_in)
    rows_own, rows_other = grads(
        core, tok, db_in, dc_in, db_far, dc_far, rows_in, cols_in, x_far, z_far, link, end, heads
    )
    rows = rows_own + lax.ppermute(rows_other, "c", CORE_SWAP)
    new_bc, new_heads, packed, square, head_square = settle(
        fire_flags, all_to_all(rows, RING), last_bc[0], last_heads[0]
    )
    on_chip = square + lax.ppermute(square, "c", CORE_SWAP)
    squares = on_ring(ring_sum(*on_ring(on_chip, "y")), "z")
    total_bc, total_heads, trigger = finish(on_ring(packed, "dp"), squares, head_square, total_bc, total_heads)
    return total_bc, total_heads, new_bc[None], new_heads[None], trigger.reshape(1)


def solution(mesh):
    split = Mesh(mesh.devices.reshape(mesh.shape["dp"], 4, 4, 2), ("dp",) + SEQ)
    rows = P("dp", SEQ, None)
    in_specs = (
        rows, rows, rows, P(), P(), P(), P(), P("dp"), rows, P("dp", None, None), P(SEQ, None), P(),
    )
    out_specs = (P(SEQ, None), P(), rows, P("dp", None, None), P("dp"))
    return jax.shard_map(local, mesh=split, in_specs=in_specs, out_specs=out_specs, check_vma=False)
```
